32 devices in a mesh: cluster: 4 (over y, core), sub: 8 (over z, x).
Axes of the slice: x: 2, y: 2, z: 4, core: 2. Of those that a mesh axis runs over, the one named last changes fastest.
Arguments:
- compliance: float32 [4, 8, 1024, 1024], P('cluster', 'sub'), may hold values from -0.078125 to 4.078125, as said below
- loads: float32 [4, 8, 1024, 256], P('cluster', 'sub'), may hold values from -6 to 6
- modes: float32 [4, 8, 32, 1024], P('cluster', 'sub'), may hold values from -1 to 1
- coarse_inverse: float32 [4, 256, 256], P('cluster', 'sub'), may hold values from -0.9 to 0.9, as said below
- face_block: int32 [4, 8, 4], replicated, may hold values from 0 to 7, as said below
- edge_rows: int32 [4, 8, 2], replicated, may hold values from 16 to 128
Outputs:
- solution: float32 [4, 8, 1024, 256], P('cluster', 'sub')
- residual: float32 [4, 8, 1024, 256], P('cluster', 'sub')
The draws below stay inside these ranges and needn't reach their ends.
Inputs may be any that keep to these rules, and one draw needn't show every extreme that they name: `compliance`: symmetric positive definite for every subdomain. `coarse_inverse`: symmetric positive definite for every cluster. `face_block`: the four faces of a subdomain lie in four different row blocks. `edge_rows`: entries of faces with no partner are not read.
All inputs are finite; a program needn't handle non-finite values.
Results may differ from the reference program's by a relative error of at most 0.00018.
Values sent between devices are 32-bit elements; how exact they have to be, the bound alone decides.
No kernel may reach another device: no remote copies, remote signals or barrier semaphores. Data moves between devices by JAX's collectives and lax.ppermute only.
A program may use at most 64 MiB of HBM per device.

```python
import jax
import jax.numpy as jnp
from jax import lax

ORDER = 1024
BLOCK = 128
MODES = 32
LOADS = 256
ITERS = 3
CMODES = 256
N_CLUSTER = 4
N_SUB = 8


def draw_compliance(key, part):
    count = N_CLUSTER * N_SUB
    keys = jax.random.split(key, count)

    def single(subkey):
        first, second = jax.random.split(subkey)
        diag = jnp.exp(jax.random.uniform(first, (ORDER,), jnp.float32, jnp.log(2.0), jnp.log(4.0)))
        noise = jnp.clip(jax.random.normal(second, (ORDER, ORDER), jnp.float32), -5.0, 5.0) * (0.5 / ORDER ** 0.5)
        return 0.5 * (noise + noise.T) + jnp.diag(diag)
    return lax.map(single, keys).reshape(N_CLUSTER, N_SUB, ORDER, ORDER)


def draw_coarse_inverse(key, part):
    keys = jax.random.split(jax.random.fold_in(key, 7), N_CLUSTER)

    def single(subkey):
        base = jnp.clip(jax.random.normal(subkey, (CMODES, CMODES), jnp.float32), -4.0, 4.0)
        gram = jnp.dot(base, base.T, precision=lax.Precision.HIGHEST) / CMODES
        return 0.05 * gram + 0.05 * jnp.eye(CMODES, dtype=jnp.float32)
    return lax.map(single, keys)


def draw_face_block(key, part):
    nblocks = ORDER // BLOCK
    scores = jax.random.randint(jax.random.fold_in(key, 11), (N_CLUSTER, N_SUB, nblocks), 0, 1 << 20)
    scores = scores * nblocks + jnp.arange(nblocks, dtype=jnp.int32)
    order = jnp.argsort(scores, axis=-1)
    return order[..., :4].astype(jnp.int32)


def with_ends(entries, key, smallest, largest):
    index_at = [jax.random.randint(jax.random.fold_in(key, axis), (), 0, length) for axis, length in enumerate(entries.shape)]
    main_axis = entries.shape.index(max(entries.shape))
    next_to = index_at[:main_axis] + [(index_at[main_axis] + 1) % entries.shape[main_axis]] + index_at[main_axis + 1:]
    return entries.at[tuple(index_at)].set(smallest).at[tuple(next_to)].set(largest)


def level_of(rng, extent, pieces, least, largest):
    level, own = 1.0, jax.random.fold_in(rng, 6)
    for axis_at, blocks in pieces:
        draws = jnp.exp(jax.random.uniform(jax.random.fold_in(own, axis_at), (blocks,), jnp.float32, least / len(pieces), largest / len(pieces)))
        level = level * jnp.repeat(draws, extent[axis_at] // blocks).reshape([-1 if axis == axis_at else 1 for axis in range(len(extent))])
    return level


def scatter_about(own_key, dims, scale, bound, cuts=(), kind=jnp.bfloat16):
    entries = jax.random.normal(own_key, dims, jnp.float32) * scale
    if len(cuts) > 0:
        entries = level_of(own_key, dims, cuts, -0.22, 0.18) * entries
    return jnp.clip(entries, min=-bound, max=bound).astype(kind)


def setup_inputs(seed: int = 0) -> dict:
    splits = jax.random.split(jax.random.key(seed), 7)
    compliance = draw_compliance(jax.random.fold_in(splits[6], 71), 0)
    loads = scatter_about(splits[1], (N_CLUSTER, N_SUB, ORDER, LOADS), 1.0, 6.0, ((0, 4), (1, 8)), jnp.float32)
    modes = scatter_about(splits[2], (N_CLUSTER, N_SUB, MODES, ORDER), MODES ** -0.5, 1.0, ((0, 4), (1, 8)), jnp.float32)
    coarse_inverse = draw_coarse_inverse(jax.random.fold_in(splits[6], 71), 0)
    face_block = draw_face_block(jax.random.fold_in(splits[6], 71), 0)
    edge_rows = with_ends(jax.random.randint(splits[5], (N_CLUSTER, N_SUB, 2), BLOCK // 8, BLOCK + 1), jax.random.fold_in(splits[5], 1), BLOCK // 8, BLOCK).astype(jnp.int32)
    return dict(compliance=compliance, loads=loads, modes=modes, coarse_inverse=coarse_inverse, face_block=face_block, edge_rows=edge_rows)


def face_values(blocks, onehot, face):
    return jnp.einsum('csb,csbrl->csrl', onehot[:, :, face, :], blocks, precision=lax.Precision.HIGHEST)


def assemble(field, face_block, edge_rows):
    nclus, nsub = field.shape[0], field.shape[1]
    nblocks = ORDER // BLOCK
    width = field.shape[-1]
    blocks = field.reshape(nclus, nsub, nblocks, BLOCK, width)
    onehot = (face_block[..., None] == jnp.arange(nblocks, dtype=jnp.int32)).astype(field.dtype)
    rows = jnp.arange(BLOCK, dtype=jnp.int32)
    values = [face_values(blocks, onehot, face) for face in range(4)]
    sub_mask = (rows < edge_rows[:, :-1, 0, None]).astype(field.dtype)[..., None]
    clus_mask = (rows < edge_rows[:-1, :, 1, None]).astype(field.dtype)[..., None]
    zero4 = (0, 0)
    added = [
        jnp.pad(0.5 * sub_mask * values[1][:, :-1], (zero4, (1, 0), zero4, zero4)),
        jnp.pad(0.5 * sub_mask * values[0][:, 1:], (zero4, (0, 1), zero4, zero4)),
        jnp.pad(0.5 * clus_mask * values[3][:-1], ((1, 0), zero4, zero4, zero4)),
        jnp.pad(0.5 * clus_mask * values[2][1:], ((0, 1), zero4, zero4, zero4)),
    ]
    total = jnp.zeros_like(blocks)
    for face in range(4):
        total = total + onehot[:, :, face, :, None, None] * added[face][:, :, None, :, :]
    return field + total.reshape(field.shape)


def local_apply(compliance, field):
    nclus, nsub = field.shape[0], field.shape[1]
    mats = compliance.reshape(nclus * nsub, ORDER, ORDER)
    vecs = field.reshape(nclus * nsub, ORDER, field.shape[-1])
    out = lax.map(lambda pair: jnp.dot(pair[0], pair[1], precision=lax.Precision.HIGHEST), (mats, vecs))
    return out.reshape(field.shape)


def operator(compliance, face_block, edge_rows, field):
    return assemble(local_apply(compliance, assemble(field, face_block, edge_rows)), face_block, edge_rows)


def precondition(modes, coarse_inverse, resid):
    nclus, nsub = resid.shape[0], resid.shape[1]
    coarse = jnp.einsum('csmo,csol->csml', modes, resid, precision=lax.Precision.HIGHEST)
    stacked = coarse.reshape(nclus, nsub * MODES, resid.shape[-1])
    solved = jnp.einsum('cij,cjl->cil', coarse_inverse, stacked, precision=lax.Precision.HIGHEST)
    solved = solved.reshape(nclus, nsub, MODES, resid.shape[-1])
    return resid + jnp.einsum('csmo,csml->csol', modes, solved, precision=lax.Precision.HIGHEST)


def column_sums(left, right):
    return jnp.sum(left * right, axis=(0, 1, 2))


def reference(compliance, loads, modes, coarse_inverse, face_block, edge_rows):
    solution = jnp.zeros_like(loads)
    residual = loads
    precond = precondition(modes, coarse_inverse, residual)
    direction = precond
    rz_now = column_sums(residual, precond)
    for step in range(ITERS):
        image = operator(compliance, face_block, edge_rows, direction)
        alpha = rz_now / column_sums(direction, image)
        solution = solution + alpha * direction
        residual = residual - alpha * image
        if step + 1 < ITERS:
            precond = precondition(modes, coarse_inverse, residual)
            rz_next = column_sums(residual, precond)
            direction = precond + (rz_next / rz_now) * direction
            rz_now = rz_next
    return solution, residual
```

```python
import jax
import jax.numpy as jnp
from jax import lax
from jax.sharding import PartitionSpec as P

BLOCK = 128
ITERS = 3
PAD = 8
HI = lax.Precision.HIGHEST


def mm(left, right):
    return jnp.dot(left, right, precision=HI, preferred_element_type=jnp.float32)


def mm_t(left, right):
    return lax.dot_general(
        left, right, (((0,), (0,)), ((), ())), precision=HI, preferred_element_type=jnp.float32
    )


def pair_list(count, parity, wrap=False):
    pairs = []
    for low in range(parity, count - 1, 2):
        pairs += [(low, low + 1), (low + 1, low)]
    if wrap and parity == 1 and count > 2:
        pairs += [(count - 1, 0), (0, count - 1)]
    return pairs


def rows_of(field, start, count=BLOCK):
    return lax.dynamic_slice_in_dim(field, start, count, 0)


def shards(compliance, loads, modes, coarse_inverse, face_block, edge_rows):
    matrix = compliance[0, 0]
    rhs = loads[0, 0]
    basis = modes[0, 0]
    inverse_rows = coarse_inverse[0]
    nmodes, order = basis.shape
    width = rhs.shape[1]
    nclus, nsub = lax.axis_size("cluster"), lax.axis_size("sub")
    clus, sub = lax.axis_index("cluster"), lax.axis_index("sub")
    faces = face_block[clus, sub]
    row_ids = jnp.arange(BLOCK, dtype=jnp.int32)

    links = []
    for axis, index, count, lower, upper, kind in (
        ("sub", sub, nsub, 0, 1, 0),
        ("cluster", clus, nclus, 2, 3, 1),
    ):
        for parity in (0, 1):
            is_low = lax.rem(index + parity, 2) == 0
            partner = jnp.where(is_low, index + 1, index - 1)
            valid = (partner >= 0) & (partner < count)
            first = jnp.clip(jnp.minimum(index, partner), 0, count - 1)
            at = (clus, first) if kind == 0 else (first, sub)
            length = jnp.where(valid, edge_rows[at[0], at[1], kind], 0)
            start = jnp.where(is_low, faces[upper], faces[lower]) * BLOCK
            mask = (row_ids < length).astype(jnp.float32)[:, None]
            links.append((axis, pair_list(count, parity), start, mask))
    order_of_sends = (1, 0, 3, 2)

    def exchange(messages):
        got = [None] * 4
        for at in order_of_sends:
            got[at] = lax.ppermute(messages[at], links[at][0], links[at][1])
        return got

    def spread(payload, axis, count):
        blocks = jnp.broadcast_to(payload[None], (count,) + payload.shape)
        return lax.all_to_all(blocks, axis, 0, 0, tiled=False)

    def mirror(ymom, doubled):
        first = lax.ppermute(ymom, "cluster", pair_list(nclus, 0))
        if doubled:
            sums = ymom[nmodes:] + first[nmodes:]
            second = lax.ppermute(
                jnp.concatenate([ymom[:nmodes], sums], 0), "cluster", pair_list(nclus, 1, True)
            )
            sums = sums + second[nmodes:]
        else:
            second = lax.ppermute(ymom[:nmodes], "cluster", pair_list(nclus, 1))
            sums = lax.psum(ymom[nmodes:], "cluster") if ymom.shape[0] > nmodes else None
        return first[:nmodes], second[:nmodes], sums

    face_modes = [lax.dynamic_slice_in_dim(basis, link[2], BLOCK, 1) for link in links]
    messages = []
    for at, link in enumerate(links):
        parts = [rows_of(rhs, link[2]), jnp.pad(face_modes[at], ((0, 0), (0, width - BLOCK)))]
        if at < 2:
            parts.append(inverse_rows.reshape(-1, width))
        messages.append(jnp.concatenate(parts, 0))
    got = exchange(messages)
    kappa = mm(basis, rhs)
    gathered = spread(kappa, "sub", nsub).reshape(nsub * nmodes, width)

    inv = [inverse_rows] + [
        got[at][BLOCK + nmodes :].reshape(inverse_rows.shape) for at in (0, 1)
    ]
    three = jnp.concatenate(inv, 0)
    padded = jnp.pad(
        three.reshape(3 * nmodes, nsub, nmodes), ((0, 0), (0, 0), (0, PAD))
    ).reshape(3 * nmodes, nsub * (nmodes + PAD))
    picks = jnp.tile(
        jnp.concatenate([jnp.zeros((PAD, nmodes), jnp.float32), jnp.eye(PAD, dtype=jnp.float32)], 1),
        (1, nsub),
    )
    gather_map = jnp.concatenate([padded[:nmodes], picks, padded[nmodes:]], 0)

    extended = [basis]
    late = []
    for at, link in enumerate(links):
        theirs = got[at][BLOCK : BLOCK + nmodes, :BLOCK]
        weight = (0.5 * link[3][:, 0])[None, :]
        extended.append(
            lax.dynamic_update_slice(
                jnp.zeros((nmodes, order), jnp.float32), weight * theirs, (0, link[2])
            )
        )
        late.append(weight * face_modes[at])
    extended = jnp.concatenate(extended, 0)
    late = jnp.concatenate(late, 1)

    def add_faces(field, blocks):
        for link, block in zip(links, blocks):
            current = rows_of(field, link[2])
            field = lax.dynamic_update_slice_in_dim(field, current + block, link[2], 0)
        return field

    y3 = mm(three, gathered)
    y_c0, y_c1, _ = mirror(y3[:nmodes], False)
    eta = y3[:nmodes]
    stack = jnp.concatenate([y3, y_c0, y_c1], 0)
    base = add_faces(rhs, [0.5 * link[3] * g[:BLOCK] for link, g in zip(links, got)])
    vee = base + mm_t(extended, stack)
    resid = rhs
    doubled = nclus == 4

    betas, alphas, resids, etas, along = [], [], [], [], None
    rz_now = None
    history = []
    for step in range(ITERS):
        image = mm(matrix, vee)
        rz_part = jnp.sum(resid * resid, 0, keepdims=True) + jnp.sum(kappa * eta, 0, keepdims=True)
        curve_part = jnp.sum(vee * image, 0, keepdims=True)
        moments = jnp.concatenate(
            [rz_part, curve_part, jnp.zeros((PAD - 2, width), jnp.float32)], 0
        )
        own = [rows_of(image, link[2]) for link in links]
        got = exchange(own)
        q_image = add_faces(image, [0.5 * link[3] * g for link, g in zip(links, got)])
        resids.append(resid)
        etas.append(eta)
        if step + 1 < ITERS:
            coarse = mm(basis, image) + mm(late, jnp.concatenate(got, 0))
            gathered = spread(jnp.concatenate([coarse, moments], 0), "sub", nsub)
            y3 = mm(gather_map, gathered.reshape(nsub * (nmodes + PAD), width))
            y_c0, y_c1, sums = mirror(y3[: nmodes + PAD], doubled)
            ynew = y3[:nmodes]
            stack = jnp.concatenate([ynew, y3[nmodes + PAD :], y_c0, y_c1], 0)
            qq = add_faces(
                image, [link[3] * (g + 0.25 * f) for link, g, f in zip(links, got, own)]
            )
            tee = qq + mm_t(extended, stack)
        else:
            everyone = spread(moments, ("cluster", "sub"), nclus * nsub)
            sums = jnp.sum(everyone, 0)
            coarse = ynew = tee = None
        rz, curve = sums[0:1], sums[1:2]
        if step == 0:
            alpha = rz / curve
            along = (q_image, coarse, ynew, tee)
        else:
            beta = rz / rz_now
            alpha = rz / (curve - beta * rz / alphas[-1])
            betas.append(beta)
            along = tuple(
                None if new is None else new + beta * old
                for new, old in zip((q_image, coarse, ynew, tee), along)
            )
        alphas.append(alpha)
        rz_now = rz
        resid = resid - alpha * along[0]
        if step + 1 < ITERS:
            kappa = kappa - alpha * along[1]
            eta = eta - alpha * along[2]
            vee = vee - alpha * along[3]

    weights = [None] * ITERS
    running = None
    for step in reversed(range(ITERS)):
        running = alphas[step] if running is None else alphas[step] + betas[step] * running
        weights[step] = running
    total = sum(w * r for w, r in zip(weights, resids))
    coarse_total = sum(w * e for w, e in zip(weights, etas))
    answer = total + mm_t(basis, coarse_total)
    return (answer[None, None], resid[None, None])


def solution(mesh):
    return jax.shard_map(
        shards,
        mesh=mesh,
        in_specs=(
            P("cluster", "sub", None, None),
            P("cluster", "sub", None, None),
            P("cluster", "sub", None, None),
            P("cluster", "sub", None),
            P(),
            P(),
        ),
        out_specs=(P("cluster", "sub", None, None), P("cluster", "sub", None, None)),
        check_vma=False,
    )
```

```python
import jax
import jax.numpy as jnp
from jax import lax
from jax.experimental import pallas as pl
from jax.experimental.pallas import tpu as pltpu
from jax.sharding import PartitionSpec as P


BLOCK = 128
ITERS = 3
PAD = 8
ROWS = 256
F32 = jnp.float32
BF16 = jnp.bfloat16
VM = pl.BlockSpec(memory_space=pltpu.VMEM)
SM = pl.BlockSpec(memory_space=pltpu.SMEM)


def sds(*shape, dtype=F32):
    return jax.ShapeDtypeStruct(shape, dtype)


def call(body, outs, args, smem_in=(), smem_out=(), flops=1_000_000, mib=8):
    outs = list(outs)
    return pl.pallas_call(
        body,
        out_shape=outs,
        in_specs=[SM if at in smem_in else VM for at in range(len(args))],
        out_specs=[SM if at in smem_out else VM for at in range(len(outs))],
        compiler_params=pltpu.CompilerParams(vmem_limit_bytes=mib << 20),
        cost_estimate=pl.CostEstimate(
            flops=flops, bytes_accessed=1 << 20, transcendentals=0),
    )(*args)


def split(value):
    high = value.astype(BF16)
    return high, (value - high.astype(F32)).astype(BF16)


def dot(left, right):
    return jnp.dot(left, right, preferred_element_type=F32)


def dot3(left, right):
    return dot(left[0], right[0]) + (dot(left[0], right[1]) + dot(left[1], right[0]))


def dot6(left, right):
    return jnp.dot(left, right, precision=lax.Precision.HIGHEST, preferred_element_type=F32)


def pair_list(count, parity, wrap=False):
    pairs = []
    for low in range(parity, count - 1, 2):
        pairs += [(low, low + 1), (low + 1, low)]
    if wrap and parity == 1 and count > 2:
        pairs += [(count - 1, 0), (0, count - 1)]
    return pairs


def half(refs, rows):
    return refs[0][rows, :], refs[1][rows, :]


def start_body(face_block, edge_rows, rhs_in, basis_in, inverse_in, *outs):
    *messages, meta, kappa, spread, rhs, basis, inverse_rows, sems = outs
    copies = [
        pltpu.make_async_copy(source, target, sems.at[at])
        for at, (source, target) in enumerate(
            ((rhs_in, rhs), (basis_in, basis), (inverse_in, inverse_rows)))
    ]
    for copy in copies:
        copy.start()
    nmodes = basis.shape[0]
    width = rhs.shape[1]
    clus, sub = lax.axis_index("cluster"), lax.axis_index("sub")
    link = 0
    for index, count, lower, upper, kind in (
        (sub, face_block.shape[2], 0, 1, 0),
        (clus, face_block.shape[0], 2, 3, 1),
    ):
        for parity in (0, 1):
            is_low = lax.rem(index + parity, 2) == 0
            partner = jnp.where(is_low, index + 1, index - 1)
            valid = (partner >= 0) & (partner < count)
            first = jnp.clip(jnp.minimum(index, partner), 0, count - 1)
            place = (clus, first) if kind == 0 else (first, sub)
            meta[link] = face_block[clus, jnp.where(is_low, upper, lower), sub] * BLOCK
            meta[4 + link] = jnp.where(valid, edge_rows[place[0], kind, place[1]], 0)
            link += 1
    for copy in copies:
        copy.wait()
    for at, message in enumerate(messages):
        start = pl.multiple_of(meta[at], BLOCK)
        message[:BLOCK] = rhs[pl.ds(start, BLOCK), :]
        message[BLOCK : BLOCK + nmodes, :BLOCK] = basis[:, pl.ds(start, BLOCK)]
        if width > BLOCK:
            message[BLOCK : BLOCK + nmodes, BLOCK:] = jnp.zeros((nmodes, width - BLOCK), F32)
        if at < 2:
            message[BLOCK + nmodes :] = inverse_rows[...]
    value = dot6(basis[...], rhs[...])
    kappa[...] = value
    for at in range(spread.shape[0]):
        spread[at] = value


def prepare_body(matrix, c_hi, c_lo):
    @pl.loop(0, matrix.shape[0] // BLOCK)
    def _(at):
        rows = pl.ds(pl.multiple_of(at * BLOCK, BLOCK), BLOCK)
        c_hi[rows, :], c_lo[rows, :] = split(matrix[rows, :])


def masks_of(starts, at, width):
    ids = lax.broadcasted_iota(jnp.int32, (BLOCK, width), 0)
    return (ids < starts[4 + at]).astype(F32)


def setup_body(starts, rhs, basis, i0, i1, gathered, g0, g1, g2, g3,
               others, b_hi, b_lo, m_hi, m_lo, l_hi, l_lo, base):
    nmodes, _ = basis.shape
    skip = i0.shape[0] - nmodes
    others[:nmodes] = dot6(i0[skip:], gathered[...])
    others[nmodes:] = dot6(i1[skip:], gathered[...])
    width = rhs.shape[1]
    base[...] = rhs[...]
    m_hi[...], m_lo[...] = split(basis[...])
    b_hi[...] = jnp.zeros_like(b_hi)
    b_lo[...] = jnp.zeros_like(b_lo)
    own = basis[...].T
    b_hi[:, :nmodes], b_lo[:, :nmodes] = split(own)
    for at, got in enumerate((g0, g1, g2, g3)):
        start = pl.multiple_of(starts[at], BLOCK)
        rows = pl.ds(start, BLOCK)
        mask = 0.5 * masks_of(starts, at, width)
        base[rows, :] = base[rows, :] + mask * got[:BLOCK, :]
        theirs = got[BLOCK : BLOCK + nmodes, :BLOCK].T
        cols = slice((at + 1) * nmodes, (at + 2) * nmodes)
        b_hi[rows, cols], b_lo[rows, cols] = split(mask[:, :nmodes] * theirs)
        ids = lax.broadcasted_iota(jnp.int32, (nmodes, BLOCK), 1)
        weight = 0.5 * (ids < starts[4 + at]).astype(F32)
        cols = slice(at * BLOCK, (at + 1) * BLOCK)
        l_hi[:, cols], l_lo[:, cols] = split(weight * basis[:, pl.ds(start, BLOCK)])


def maps_body(c_hi, c_lo, b_hi, b_lo, k_hi, k_lo):
    k_hi[...], k_lo[...] = split(dot3((c_hi[...], c_lo[...]), (b_hi[...], b_lo[...])))


def copy_faces(starts, field, outs):
    for at, out in enumerate(outs):
        out[...] = field[pl.ds(pl.multiple_of(starts[at], BLOCK), BLOCK), :]


def first_y_body(inverse_rows, gathered, own):
    own[...] = dot6(inverse_rows[...], gathered[...])


def fold_body(everyone, out):
    total = everyone[0]
    for at in range(1, everyone.shape[0]):
        total = total + everyone[at]
    out[...] = total


def stacked(own, others, first, second):
    nmodes = others.shape[0] // 2
    return jnp.concatenate([own[:nmodes], others[...], first[:nmodes], second[:nmodes]], 0)


def first_apply_body(starts, base, c_hi, c_lo, b_hi, b_lo, own, others, first, second,
                     vee, image, *outs):
    ys = split(stacked(own, others, first, second))

    @pl.loop(0, base.shape[0] // ROWS)
    def _(at):
        rows = pl.ds(pl.multiple_of(at * ROWS, ROWS), ROWS)
        vee[rows, :] = base[rows, :] + dot3(half((b_hi, b_lo), rows), ys)

    image[...] = dot3((c_hi[...], c_lo[...]), split(vee[...]))

    copy_faces(starts, image, outs)


def column_sum(total):
    return jnp.sum(total, 0, keepdims=True)


def moment_rows(vee, image, resid, kappa, eta):
    width = resid.shape[1]

    def step(at, carry):
        rows = pl.ds(pl.multiple_of(at * BLOCK, BLOCK), BLOCK)
        value = resid[rows, :]
        squares = (value * value).reshape(-1, 8, width)
        curves = (vee[rows, :] * image[rows, :]).reshape(-1, 8, width)
        return carry[0] + jnp.sum(squares, 0), carry[1] + jnp.sum(curves, 0)

    zero = jnp.zeros((8, width), F32)
    rr, curve = lax.fori_loop(0, resid.shape[0] // BLOCK, step, (zero, zero))
    rz = column_sum(rr) + column_sum(kappa[...] * eta[...])
    curve = column_sum(curve)
    ids = lax.broadcasted_iota(jnp.int32, (PAD, width), 0)
    return jnp.where(ids == 0, rz, 0.0) + jnp.where(ids == 1, curve, 0.0)


def sums_body(m_hi, m_lo, vee, image, resid, kappa, eta, out):
    nmodes = kappa.shape[0]
    out[nmodes:] = moment_rows(vee, image, resid, kappa, eta)
    out[:nmodes] = dot3((m_hi[...], m_lo[...]), split(image[...]))


def coarse_late_body(main, l_hi, l_lo, g0, g1, g2, g3, spread):
    nmodes = l_hi.shape[0]
    total = main[:nmodes]
    for at, got in enumerate((g0, g1, g2, g3)):
        cols = slice(at * BLOCK, (at + 1) * BLOCK)
        total = total + dot3((l_hi[:, cols], l_lo[:, cols]), split(got[...]))
    for at in range(spread.shape[0]):
        spread[at, :nmodes] = total
        spread[at, nmodes:] = main[nmodes:]


def faces_body(starts, image, c_hi, c_lo, g0, g1, g2, g3, qonce, qtwice, prod):
    width = image.shape[1]
    qonce[...] = image[...]
    qtwice[...] = image[...]
    for at, got in enumerate((g0, g1, g2, g3)):
        rows = pl.ds(pl.multiple_of(starts[at], BLOCK), BLOCK)
        mask = masks_of(starts, at, width)
        mine = image[rows, :]
        qonce[rows, :] = mine + (0.5 * mask) * got[...]
        qtwice[rows, :] = mine + mask * (got[...] + 0.25 * mine)
    prod[...] = dot3((c_hi[...], c_lo[...]), split(qtwice[...]))


def y_body(inverse_rows, i0, i1, gathered, own, others, coarse):
    count, rows, _ = gathered.shape
    nmodes = rows - PAD
    blocks = jnp.concatenate([gathered[at, :nmodes] for at in range(count)], 0)
    own[:nmodes] = dot6(inverse_rows[...], blocks)
    skip = i0.shape[0] - nmodes
    others[:nmodes] = dot6(i0[skip:], blocks)
    others[nmodes:] = dot6(i1[skip:], blocks)
    total = gathered[0, nmodes:]
    for at in range(1, count):
        total = total + gathered[at, nmodes:]
    own[nmodes:] = total
    me = lax.axis_index("sub")
    coarse[...] = gathered[me, :nmodes]


def scalars(sums, rz_old, alpha_old):
    rz, curve = sums[0:1], sums[1:2]
    if rz_old is None:
        return rz / curve, None, rz
    beta = rz / rz_old
    return rz / (curve - beta * rz / alpha_old), beta, rz


def pack(alpha, beta, rz):
    ids = lax.broadcasted_iota(jnp.int32, (PAD, alpha.shape[1]), 0)
    out = jnp.where(ids == 0, alpha, 0.0) + jnp.where(ids == 2, rz, 0.0)
    return out if beta is None else out + jnp.where(ids == 1, beta, 0.0)


def make_image_body(has_old):
    def body(starts, image, prod, k_hi, k_lo, own, others, first, second, *rest):
        *rest, f0, f1, f2, f3 = rest
        nmodes = others.shape[0] // 2
        sums = own[nmodes:] + first[nmodes:] + second[nmodes:]
        if has_old:
            scal_old, along_old, image_new, along, scal = rest
            alpha, beta, rz = scalars(sums, scal_old[2:3], scal_old[0:1])
        else:
            image_new, along, scal = rest
            alpha, beta, rz = scalars(sums, None, None)
        scal[...] = pack(alpha, beta, rz)
        ys = split(stacked(own, others, first, second))

        @pl.loop(0, image.shape[0] // ROWS)
        def _(at):
            rows = pl.ds(pl.multiple_of(at * ROWS, ROWS), ROWS)
            value = prod[rows, :] + dot3(half((k_hi, k_lo), rows), ys)
            if has_old:
                value = value + beta * along_old[rows, :]
            along[rows, :] = value
            image_new[rows, :] = image[rows, :] - alpha * value

        copy_faces(starts, image_new, (f0, f1, f2, f3))

    return body


def make_update_body(has_old, last):
    def body(scal, vee, qtwice, b_hi, b_lo, own, others, first, second,
             resid, qonce, kappa, coarse, eta, image, m_hi, m_lo, *rest):
        if has_old:
            t_old, q_old, k_old, y_old = rest[:4]
            rest = rest[4:]
        vee_new, resid_new, kappa_new, eta_new, t_along, q_along, k_along, y_along, out = rest
        alpha, beta = scal[0:1], scal[1:2]
        nmodes = kappa.shape[0]
        ys = split(stacked(own, others, first, second))

        def move(old, value, older):
            if has_old:
                value = value + beta * older
            return value, old - alpha * value

        @pl.loop(0, vee.shape[0] // ROWS)
        def _(at):
            rows = pl.ds(pl.multiple_of(at * ROWS, ROWS), ROWS)
            value = qtwice[rows, :] + dot3(half((b_hi, b_lo), rows), ys)
            t_along[rows, :], vee_new[rows, :] = move(
                vee[rows, :], value, t_old[rows, :] if has_old else None)
            q_along[rows, :], resid_new[rows, :] = move(
                resid[rows, :], qonce[rows, :], q_old[rows, :] if has_old else None)

        k_along[...], kappa_new[...] = move(kappa[...], coarse[...], k_old[...] if has_old else None)
        y_along[...], eta_new[...] = move(eta[...], own[:nmodes], y_old[...] if has_old else None)
        moments = moment_rows(vee_new, image, resid_new, kappa_new, eta_new)
        if last:
            for at in range(out.shape[0]):
                out[at] = moments
        else:
            out[:nmodes] = dot3((m_hi[...], m_lo[...]), split(image[...]))
            out[nmodes:] = moments

    return body


def finish_body(starts, sums, scal0, scal1, b_hi, b_lo, e0, e1, e2, r0, r1, r2, along, image,
                g0, g1, g2, g3, answer, resid):
    at = pl.program_id(0)
    rows = pl.ds(pl.multiple_of(at * ROWS, ROWS), ROWS)
    nmodes = e0.shape[0]
    width = r0.shape[1]
    alpha, beta, _ = scalars(sums[...], scal1[2:3], scal1[0:1])
    a1 = scal1[0:1] + beta * alpha
    a0 = scal0[0:1] + scal1[1:2] * a1
    ys = split(a0 * e0[...] + a1 * e1[...] + alpha * e2[...])
    maps = (b_hi[rows, :nmodes], b_lo[rows, :nmodes])
    last = r2[rows, :]
    answer[...] = a0 * r0[rows, :] + a1 * r1[rows, :] + alpha * last + dot3(maps, ys)
    resid[...] = last - alpha * (image[rows, :] + beta * along[rows, :])
    for which, got in enumerate((g0, g1, g2, g3)):
        offset = starts[which] - at * ROWS

        @pl.when((offset >= 0) & (offset < ROWS))
        def _(which=which, got=got, offset=offset):
            part = pl.ds(pl.multiple_of(offset, BLOCK), BLOCK)
            mask = (0.5 * masks_of(starts, which, width)) * alpha
            resid[part, :] = resid[part, :] - mask * got[...]


def shards(compliance, loads, modes, coarse_inverse, face_block, edge_rows):
    matrix = compliance[0, 0]
    rhs = loads[0, 0]
    basis = modes[0, 0]
    inverse_rows = coarse_inverse[0]
    nmodes, order = basis.shape
    width = rhs.shape[1]
    coarse_all = inverse_rows.shape[1]
    nclus, nsub = lax.axis_size("cluster"), lax.axis_size("sub")
    full = sds(order, width)
    small = sds(nmodes, width)
    block = sds(BLOCK, width)
    tall = 5 * nmodes
    doubled = nclus == 4

    links = [("sub", pair_list(nsub, parity)) for parity in (0, 1)]
    links += [("cluster", pair_list(nclus, parity)) for parity in (0, 1)]

    def exchange(messages):
        got = [None] * 4
        for at in (1, 0, 3, 2):
            got[at] = lax.ppermute(messages[at], links[at][0], links[at][1])
        return got

    def gather(blocks, axis="sub"):
        return lax.all_to_all(blocks, axis, 0, 0, tiled=False)

    def mirror(ymom):
        first = lax.ppermute(ymom, "cluster", pair_list(nclus, 0))
        if doubled:
            sums = ymom[nmodes:] + first[nmodes:]
            both = jnp.concatenate([ymom[:nmodes], sums], 0)
            second = lax.ppermute(both, "cluster", pair_list(nclus, 1, True))
            return first, second
        mine = ymom[nmodes:]
        rest = lax.psum(mine, "cluster") - mine
        second = lax.ppermute(ymom[:nmodes], "cluster", pair_list(nclus, 1))
        return (
            jnp.concatenate([first[:nmodes], rest], 0),
            jnp.concatenate([second, jnp.zeros_like(rest)], 0),
        )

    extra = nmodes * coarse_all // width
    sizes = [BLOCK + nmodes + (extra if at < 2 else 0) for at in range(4)]
    anywhere = pl.BlockSpec(memory_space=pl.ANY)
    *messages, meta, kappa, spread = pl.pallas_call(
        start_body,
        out_shape=[sds(size, width) for size in sizes]
        + [sds(8, dtype=jnp.int32), small, sds(nsub, nmodes, width)],
        in_specs=[SM, SM, anywhere, anywhere, anywhere],
        out_specs=[VM] * 4 + [SM, VM, VM],
        scratch_shapes=[
            pltpu.VMEM((order, width), F32),
            pltpu.VMEM((nmodes, order), F32),
            pltpu.VMEM((extra, width), F32),
            pltpu.SemaphoreType.DMA((3,)),
        ],
        compiler_params=pltpu.CompilerParams(vmem_limit_bytes=16 << 20),
        name="start",
    )(face_block.swapaxes(1, 2), edge_rows.swapaxes(1, 2), rhs, basis,
      inverse_rows.reshape(extra, width))
    got = exchange(messages)
    gathered = gather(spread).reshape(nsub * nmodes, width)
    c_pair = call(
        prepare_body, [sds(order, order, dtype=BF16)] * 2, [matrix],
        flops=10_000_000)
    inverses = [inverse_rows, *got[:2]]
    if coarse_all != width:
        inverses[1:] = [each[BLOCK + nmodes :].reshape(nmodes, coarse_all) for each in got[:2]]
    own = call(first_y_body, [small], [inverse_rows, gathered])[0]
    first = lax.ppermute(own, "cluster", pair_list(nclus, 0))
    second = lax.ppermute(own, "cluster", pair_list(nclus, 1))
    mapping = sds(order, tall, dtype=BF16)
    thin = sds(nmodes, order, dtype=BF16)
    lates = sds(nmodes, 4 * BLOCK, dtype=BF16)
    others, *pairs, base = call(
        setup_body,
        [sds(2 * nmodes, width), mapping, mapping, thin, thin, lates, lates, full],
        [meta, rhs, basis, *inverses[1:], gathered, *got], smem_in=(0,),
        flops=100_000_000)
    b_pair, m_pair, l_pair = pairs[0:2], pairs[2:4], pairs[4:6]
    vee, image, *own_faces = call(
        first_apply_body, [full, full] + [block] * 4,
        [meta, base, *c_pair, *b_pair, own, others, first, second], smem_in=(0,))
    resid, eta = rhs, own

    resids, etas, scals = [resid], [eta], []
    along = None
    u_along = None
    for step in range(ITERS - 1):
        got = exchange(own_faces)
        if step == 0:
            main = call(sums_body, [sds(nmodes + PAD, width)],
                        [*m_pair, vee, image, resid, kappa, eta])[0]
            k_pair = call(maps_body, [mapping, mapping], [*c_pair, *b_pair],
                          flops=50_000_000)
        else:
            vee, resid, kappa, eta, *along, main = update(False)
            resids.append(resid)
            etas.append(eta)
        spread = call(coarse_late_body, [sds(nsub, nmodes + PAD, width)],
                      [main, *l_pair, *got])[0]
        gathered = gather(spread)
        qonce, qtwice, prod = call(
            faces_body, [full, full, full], [meta, image, *c_pair, *got],
            smem_in=(0,), flops=100_000_000)
        own, others, coarse = call(
            y_body, [sds(nmodes + PAD, width), sds(2 * nmodes, width), small],
            [*inverses, gathered])
        first, second = mirror(own)
        old = step > 0
        image_new, u_along, scal, *own_faces = call(
            make_image_body(old), [full, full, sds(PAD, width)] + [block] * 4,
            [meta, image, prod, *k_pair, own, others, first, second]
            + ([scals[-1], u_along] if old else []), smem_in=(0,))
        scals.append(scal)

        def update(last, scal=scal, vee=vee, qtwice=qtwice, own=own, others=others, first=first,
                   second=second, resid=resid, qonce=qonce, kappa=kappa, coarse=coarse, eta=eta,
                   image_new=image_new, along=along, old=old):
            out = sds(nclus * nsub, PAD, width) if last else sds(nmodes + PAD, width)
            return call(
                make_update_body(old, last),
                [full, full, small, small, full, full, small, small, out],
                [scal, vee, qtwice, *b_pair, own, others, first, second, resid, qonce, kappa,
                 coarse, eta, image_new, *m_pair] + (list(along) if old else []))

        image = image_new

    vee, resid, kappa, eta, *along, main = update(True)
    resids.append(resid)
    etas.append(eta)
    got = exchange(own_faces)
    sums = call(fold_body, [sds(PAD, width)], [gather(main, ("cluster", "sub"))])[0]
    args = [meta, sums, *scals, *b_pair, *etas, *resids, along[1], image, *got]
    answer, resid = pl.pallas_call(
        finish_body,
        grid=(order // ROWS,),
        out_shape=[full, full],
        in_specs=[SM] + [VM] * (len(args) - 1),
        out_specs=[pl.BlockSpec((ROWS, width), lambda at: (at, 0))] * 2,
        compiler_params=pltpu.CompilerParams(vmem_limit_bytes=8 << 20),
        cost_estimate=pl.CostEstimate(
            flops=1_000_000, bytes_accessed=1 << 20, transcendentals=0),
        name="finish",
    )(*args)
    return (answer[None, None], resid[None, None])


def solution(mesh):
    return jax.shard_map(
        shards,
        mesh=mesh,
        in_specs=(
            P("cluster", "sub", None, None),
            P("cluster", "sub", None, None),
            P("cluster", "sub", None, None),
            P("cluster", "sub", None),
            P(),
            P(),
        ),
        out_specs=(P("cluster", "sub", None, None), P("cluster", "sub", None, None)),
        check_vma=False,
    )
```

```python
import jax
import jax.numpy as jnp
from jax import lax
from jax.experimental import pallas as pl
from jax.experimental.pallas import tpu as pltpu
from jax.sharding import PartitionSpec as P


BLOCK = 128
ITERS = 3
PAD = 8
ROWS = 256
F32 = jnp.float32
BF16 = jnp.bfloat16
VM = pl.BlockSpec(memory_space=pltpu.VMEM)
SM = pl.BlockSpec(memory_space=pltpu.SMEM)


def sds(*shape, dtype=F32):
    return jax.ShapeDtypeStruct(shape, dtype)


def call(body, outs, args, smem_in=(), smem_out=(), flops=1_000_000, mib=8,
         scratch=()):
    outs = list(outs)
    return pl.pallas_call(
        body,
        out_shape=outs,
        in_specs=[SM if at in smem_in else VM for at in range(len(args))],
        out_specs=[SM if at in smem_out else VM for at in range(len(outs))],
        scratch_shapes=list(scratch),
        compiler_params=pltpu.CompilerParams(vmem_limit_bytes=mib << 20),
        cost_estimate=pl.CostEstimate(
            flops=flops, bytes_accessed=1 << 20, transcendentals=0),
    )(*args)


def split(value):
    high = value.astype(BF16)
    return high, (value - high.astype(F32)).astype(BF16)


def dot(left, right):
    return jnp.dot(left, right, preferred_element_type=F32)


def dot3(left, right):
    return dot(left[0], right[0]) + (dot(left[0], right[1]) + dot(left[1], right[0]))


def dot_thin(left, right):
    high, low = left
    rows = high.shape[0]
    both = dot(jnp.concatenate([high, low], 0), right[0])
    return both[:rows] + (dot(high, right[1]) + both[rows:])


def dot6(left, right):
    return jnp.dot(left, right, precision=lax.Precision.HIGHEST, preferred_element_type=F32)


def pair_list(count, parity, wrap=False):
    pairs = []
    for low in range(parity, count - 1, 2):
        pairs += [(low, low + 1), (low + 1, low)]
    if wrap and parity == 1 and count > 2:
        pairs += [(count - 1, 0), (0, count - 1)]
    return pairs


def half(refs, rows):
    return refs[0][rows, :], refs[1][rows, :]


def start_body(face_in, edge_in, rhs_in, basis_in, inverse_in, *outs):
    *messages, meta, kappa, spread, rhs, basis, inverse_rows, face_block, edge_rows, sems = outs
    copies = [
        pltpu.make_async_copy(source, target, sems.at[at])
        for at, (source, target) in enumerate(
            ((face_in, face_block), (edge_in, edge_rows), (rhs_in, rhs), (basis_in, basis),
             (inverse_in, inverse_rows)))
    ]
    for copy in copies:
        copy.start()
    for copy in copies[:2]:
        copy.wait()
    nmodes = basis.shape[0]
    width = rhs.shape[1]
    clus, sub = lax.axis_index("cluster"), lax.axis_index("sub")
    link = 0
    for index, count, lower, upper, kind in (
        (sub, face_block.shape[2], 0, 1, 0),
        (clus, face_block.shape[0], 2, 3, 1),
    ):
        for parity in (0, 1):
            is_low = lax.rem(index + parity, 2) == 0
            partner = jnp.where(is_low, index + 1, index - 1)
            valid = (partner >= 0) & (partner < count)
            first = jnp.clip(jnp.minimum(index, partner), 0, count - 1)
            place = (clus, first) if kind == 0 else (first, sub)
            meta[link] = face_block[clus, jnp.where(is_low, upper, lower), sub] * BLOCK
            meta[4 + link] = jnp.where(valid, edge_rows[place[0], kind, place[1]], 0)
            link += 1
    for copy in copies[2:]:
        copy.wait()
    for at, message in enumerate(messages):
        start = pl.multiple_of(meta[at], BLOCK)
        message[:BLOCK] = rhs[pl.ds(start, BLOCK), :]
        message[BLOCK : BLOCK + nmodes, :BLOCK] = basis[:, pl.ds(start, BLOCK)]
        if width > BLOCK:
            message[BLOCK : BLOCK + nmodes, BLOCK:] = jnp.zeros((nmodes, width - BLOCK), F32)
        if at < 2:
            message[BLOCK + nmodes :] = inverse_rows[...]
    value = dot_thin(split(basis[...]), split(rhs[...]))
    kappa[...] = value
    for at in range(spread.shape[0]):
        spread[at] = value


def masks_of(starts, at, width):
    ids = lax.broadcasted_iota(jnp.int32, (BLOCK, width), 0)
    return (ids < starts[4 + at]).astype(F32)


def setup_body(starts, matrix, rhs, basis, i0, i1, gathered, g0, g1, g2, g3,
               others, b_hi, b_lo, m_hi, m_lo, l_hi, l_lo, base, c_hi, c_lo, held, sems):
    nmodes, order = basis.shape
    parts = [pl.ds(at * ROWS, ROWS) for at in range(order // ROWS)]
    copies = [
        pltpu.make_async_copy(matrix.at[part], held.at[part], sems.at[at])
        for at, part in enumerate(parts)
    ]
    for copy in copies:
        copy.start()
    skip = i0.shape[0] - nmodes
    others[:nmodes] = dot6(i0[skip:], gathered[...])
    others[nmodes:] = dot6(i1[skip:], gathered[...])
    width = rhs.shape[1]
    base[...] = rhs[...]
    m_hi[...], m_lo[...] = split(basis[...])
    b_hi[...] = jnp.zeros_like(b_hi)
    b_lo[...] = jnp.zeros_like(b_lo)
    own = basis[...].T
    b_hi[:, :nmodes], b_lo[:, :nmodes] = split(own)
    for at, got in enumerate((g0, g1, g2, g3)):
        start = pl.multiple_of(starts[at], BLOCK)
        rows = pl.ds(start, BLOCK)
        mask = 0.5 * masks_of(starts, at, width)
        base[rows, :] = base[rows, :] + mask * got[:BLOCK, :]
        theirs = got[BLOCK : BLOCK + nmodes, :BLOCK].T
        cols = slice((at + 1) * nmodes, (at + 2) * nmodes)
        b_hi[rows, cols], b_lo[rows, cols] = split(mask[:, :nmodes] * theirs)
        ids = lax.broadcasted_iota(jnp.int32, (nmodes, BLOCK), 1)
        weight = 0.5 * (ids < starts[4 + at]).astype(F32)
        cols = slice(at * BLOCK, (at + 1) * BLOCK)
        l_hi[:, cols], l_lo[:, cols] = split(weight * basis[:, pl.ds(start, BLOCK)])
    for part, copy in zip(parts, copies):
        copy.wait()

        @pl.loop(0, ROWS // 64)
        def _(at, part=part):
            rows = pl.ds(pl.multiple_of(part.start + at * 64, 64), 64)
            c_hi[rows, :], c_lo[rows, :] = split(held[rows, :])


def maps_body(c_hi, c_lo, b_hi, b_lo, k_hi, k_lo):
    k_hi[...], k_lo[...] = split(dot3((c_hi[...], c_lo[...]), (b_hi[...], b_lo[...])))


def copy_faces(starts, field, outs):
    for at, out in enumerate(outs):
        out[...] = field[pl.ds(pl.multiple_of(starts[at], BLOCK), BLOCK), :]


def first_y_body(inverse_rows, gathered, own):
    own[...] = dot6(inverse_rows[...], gathered[...])


def fold_body(everyone, out):
    total = everyone[0]
    for at in range(1, everyone.shape[0]):
        total = total + everyone[at]
    out[...] = total


def stacked(own, others, first, second):
    nmodes = others.shape[0] // 2
    return jnp.concatenate([own[:nmodes], others[...], first[:nmodes], second[:nmodes]], 0)


def first_apply_body(starts, base, c_hi, c_lo, b_hi, b_lo, own, others, first, second,
                     vee, image, *outs):
    ys = split(stacked(own, others, first, second))

    @pl.loop(0, base.shape[0] // ROWS)
    def _(at):
        rows = pl.ds(pl.multiple_of(at * ROWS, ROWS), ROWS)
        vee[rows, :] = base[rows, :] + dot3(half((b_hi, b_lo), rows), ys)

    image[...] = dot3((c_hi[...], c_lo[...]), split(vee[...]))

    copy_faces(starts, image, outs)


def column_sum(total):
    return jnp.sum(total, 0, keepdims=True)


def moment_rows(vee, image, resid, kappa, eta):
    width = resid.shape[1]

    def step(at, carry):
        rows = pl.ds(pl.multiple_of(at * BLOCK, BLOCK), BLOCK)
        value = resid[rows, :]
        squares = (value * value).reshape(-1, 8, width)
        curves = (vee[rows, :] * image[rows, :]).reshape(-1, 8, width)
        return carry[0] + jnp.sum(squares, 0), carry[1] + jnp.sum(curves, 0)

    zero = jnp.zeros((8, width), F32)
    rr, curve = lax.fori_loop(0, resid.shape[0] // BLOCK, step, (zero, zero))
    rz = column_sum(rr) + column_sum(kappa[...] * eta[...])
    curve = column_sum(curve)
    ids = lax.broadcasted_iota(jnp.int32, (PAD, width), 0)
    return jnp.where(ids == 0, rz, 0.0) + jnp.where(ids == 1, curve, 0.0)


def sums_body(m_hi, m_lo, vee, image, resid, kappa, eta, out):
    nmodes = kappa.shape[0]
    out[nmodes:] = moment_rows(vee, image, resid, kappa, eta)
    out[:nmodes] = dot_thin((m_hi[...], m_lo[...]), split(image[...]))


def coarse_late_body(main, l_hi, l_lo, g0, g1, g2, g3, spread):
    nmodes = l_hi.shape[0]
    total = main[:nmodes]
    for at, got in enumerate((g0, g1, g2, g3)):
        cols = slice(at * BLOCK, (at + 1) * BLOCK)
        total = total + dot_thin((l_hi[:, cols], l_lo[:, cols]), split(got[...]))
    for at in range(spread.shape[0]):
        spread[at, :nmodes] = total
        spread[at, nmodes:] = main[nmodes:]


def faces_body(starts, image, c_hi, c_lo, g0, g1, g2, g3, qonce, qtwice, prod):
    width = image.shape[1]
    qonce[...] = image[...]
    qtwice[...] = image[...]
    for at, got in enumerate((g0, g1, g2, g3)):
        rows = pl.ds(pl.multiple_of(starts[at], BLOCK), BLOCK)
        mask = masks_of(starts, at, width)
        mine = image[rows, :]
        qonce[rows, :] = mine + (0.5 * mask) * got[...]
        qtwice[rows, :] = mine + mask * (got[...] + 0.25 * mine)
    prod[...] = dot3((c_hi[...], c_lo[...]), split(qtwice[...]))


def y_body(inverse_rows, i0, i1, gathered, own, others, coarse):
    count, rows, _ = gathered.shape
    nmodes = rows - PAD
    blocks = jnp.concatenate([gathered[at, :nmodes] for at in range(count)], 0)
    skip = i0.shape[0] - nmodes
    value = dot6(jnp.concatenate([inverse_rows[...], i0[skip:], i1[skip:]], 0), blocks)
    own[:nmodes] = value[:nmodes]
    others[...] = value[nmodes:]
    total = gathered[0, nmodes:]
    for at in range(1, count):
        total = total + gathered[at, nmodes:]
    own[nmodes:] = total
    me = lax.axis_index("sub")
    coarse[...] = gathered[me, :nmodes]


def scalars(sums, rz_old, alpha_old):
    rz, curve = sums[0:1], sums[1:2]
    if rz_old is None:
        return rz / curve, None, rz
    beta = rz / rz_old
    return rz / (curve - beta * rz / alpha_old), beta, rz


def pack(alpha, beta, rz):
    ids = lax.broadcasted_iota(jnp.int32, (PAD, alpha.shape[1]), 0)
    out = jnp.where(ids == 0, alpha, 0.0) + jnp.where(ids == 2, rz, 0.0)
    return out if beta is None else out + jnp.where(ids == 1, beta, 0.0)


def make_image_body(has_old):
    def body(starts, image, prod, k_hi, k_lo, own, others, first, second, *rest):
        *rest, f0, f1, f2, f3 = rest
        nmodes = others.shape[0] // 2
        sums = own[nmodes:] + first[nmodes:] + second[nmodes:]
        if has_old:
            scal_old, along_old, image_new, scal = rest
            alpha, beta, rz = scalars(sums, scal_old[2:3], scal_old[0:1])
        else:
            image_new, along, scal = rest
            alpha, beta, rz = scalars(sums, None, None)
        scal[...] = pack(alpha, beta, rz)
        ys = split(stacked(own, others, first, second))

        @pl.loop(0, image.shape[0] // ROWS)
        def _(at):
            rows = pl.ds(pl.multiple_of(at * ROWS, ROWS), ROWS)
            value = prod[rows, :] + dot3(half((k_hi, k_lo), rows), ys)
            if has_old:
                value = value + beta * along_old[rows, :]
            if not has_old:
                along[rows, :] = value
            image_new[rows, :] = image[rows, :] - alpha * value

        copy_faces(starts, image_new, (f0, f1, f2, f3))

    return body


def make_update_body(has_old, last):
    def body(scal, vee, qtwice, b_hi, b_lo, own, others, first, second,
             resid, qonce, kappa, coarse, eta, image, m_hi, m_lo, *rest):
        if has_old:
            t_old, q_old, k_old, y_old = rest[:4]
            rest = rest[4:]
        if last:
            resid_new, eta_new, q_along, out, vee_new, kappa_new = rest
            t_along = k_along = y_along = None
        else:
            vee_new, resid_new, kappa_new, eta_new, t_along, q_along, k_along, y_along, out = rest
        alpha, beta = scal[0:1], scal[1:2]
        nmodes = kappa.shape[0]
        ys = split(stacked(own, others, first, second))

        def move(old, value, older):
            if has_old:
                value = value + beta * older
            return value, old - alpha * value

        @pl.loop(0, vee.shape[0] // ROWS)
        def _(at):
            rows = pl.ds(pl.multiple_of(at * ROWS, ROWS), ROWS)
            value = qtwice[rows, :] + dot3(half((b_hi, b_lo), rows), ys)
            value, vee_new[rows, :] = move(
                vee[rows, :], value, t_old[rows, :] if has_old else None)
            if not last:
                t_along[rows, :] = value
            q_along[rows, :], resid_new[rows, :] = move(
                resid[rows, :], qonce[rows, :], q_old[rows, :] if has_old else None)

        k_value, kappa_new[...] = move(kappa[...], coarse[...], k_old[...] if has_old else None)
        y_value, eta_new[...] = move(eta[...], own[:nmodes], y_old[...] if has_old else None)
        if not last:
            k_along[...], y_along[...] = k_value, y_value
        moments = moment_rows(vee_new, image, resid_new, kappa_new, eta_new)
        if last:
            for at in range(out.shape[0]):
                out[at] = moments[: out.shape[1]]
        else:
            out[:nmodes] = dot_thin((m_hi[...], m_lo[...]), split(image[...]))
            out[nmodes:] = moments

    return body


def finish_body(starts, sums, scal0, scal1, b_hi, b_lo, e0, e1, e2, r0, r1, r2, along, image,
                g0, g1, g2, g3, answer, resid):
    at = pl.program_id(0)
    rows = pl.ds(pl.multiple_of(at * ROWS, ROWS), ROWS)
    nmodes = e0.shape[0]
    width = r0.shape[1]
    alpha, beta, _ = scalars(sums[...], scal1[2:3], scal1[0:1])
    a1 = scal1[0:1] + beta * alpha
    a0 = scal0[0:1] + scal1[1:2] * a1
    ys = split(a0 * e0[...] + a1 * e1[...] + alpha * e2[...])
    maps = (b_hi[rows, :nmodes], b_lo[rows, :nmodes])
    last = r2[rows, :]
    answer[...] = a0 * r0[rows, :] + a1 * r1[rows, :] + alpha * last + dot3(maps, ys)
    resid[...] = last - alpha * (image[rows, :] + beta * along[rows, :])
    for which, got in enumerate((g0, g1, g2, g3)):
        offset = starts[which] - at * ROWS

        @pl.when((offset >= 0) & (offset < ROWS))
        def _(which=which, got=got, offset=offset):
            part = pl.ds(pl.multiple_of(offset, BLOCK), BLOCK)
            mask = (0.5 * masks_of(starts, which, width)) * alpha
            resid[part, :] = resid[part, :] - mask * got[...]


def shards(compliance, loads, modes, coarse_inverse, face_block, edge_rows):
    matrix = compliance[0, 0]
    rhs = loads[0, 0]
    basis = modes[0, 0]
    inverse_rows = coarse_inverse[0]
    nmodes, order = basis.shape
    width = rhs.shape[1]
    coarse_all = inverse_rows.shape[1]
    nclus, nsub = lax.axis_size("cluster"), lax.axis_size("sub")
    full = sds(order, width)
    small = sds(nmodes, width)
    block = sds(BLOCK, width)
    tall = 5 * nmodes
    doubled = nclus == 4

    links = [("sub", pair_list(nsub, parity)) for parity in (0, 1)]
    links += [("cluster", pair_list(nclus, parity)) for parity in (0, 1)]

    def exchange(messages):
        got = [None] * 4
        for at in (1, 0, 3, 2):
            got[at] = lax.ppermute(messages[at], links[at][0], links[at][1])
        return got

    def gather(blocks, axis="sub"):
        return lax.all_to_all(blocks, axis, 0, 0, tiled=False)

    def mirror(ymom):
        first = lax.ppermute(ymom, "cluster", pair_list(nclus, 0))
        if doubled:
            sums = ymom[nmodes:] + first[nmodes:]
            both = jnp.concatenate([ymom[:nmodes], sums], 0)
            second = lax.ppermute(both, "cluster", pair_list(nclus, 1, True))
            return first, second
        mine = ymom[nmodes:]
        rest = lax.psum(mine, "cluster") - mine
        second = lax.ppermute(ymom[:nmodes], "cluster", pair_list(nclus, 1))
        return (
            jnp.concatenate([first[:nmodes], rest], 0),
            jnp.concatenate([second, jnp.zeros_like(rest)], 0),
        )

    extra = nmodes * coarse_all // width
    sizes = [BLOCK + nmodes + (extra if at < 2 else 0) for at in range(4)]
    far = pl.BlockSpec(memory_space=pltpu.HBM)
    *messages, meta, kappa, spread, rhs, basis, flat = pl.pallas_call(
        start_body,
        out_shape=[sds(size, width) for size in sizes]
        + [sds(8, dtype=jnp.int32), small, sds(nsub, nmodes, width), full,
           sds(nmodes, order), sds(extra, width)],
        in_specs=[far] * 5,
        out_specs=[VM] * 4 + [SM] + [VM] * 5,
        scratch_shapes=[
            pltpu.SMEM((nclus, 4, nsub), jnp.int32),
            pltpu.SMEM((nclus, 2, nsub), jnp.int32),
            pltpu.SemaphoreType.DMA((5,)),
        ],
        compiler_params=pltpu.CompilerParams(vmem_limit_bytes=16 << 20),
        name="start",
    )(*(pltpu.with_memory_space_constraint(each, pltpu.HBM) for each in (
        face_block.swapaxes(1, 2), edge_rows.swapaxes(1, 2), rhs, basis,
        inverse_rows.reshape(extra, width))))
    if coarse_all == width:
        inverse_rows = flat
    got = exchange(messages)
    gathered = gather(spread).reshape(nsub * nmodes, width)
    inverses = [inverse_rows, *got[:2]]
    if coarse_all != width:
        inverses[1:] = [each[BLOCK + nmodes :].reshape(nmodes, coarse_all) for each in got[:2]]
    own = call(first_y_body, [small], [inverse_rows, gathered])[0]
    first = lax.ppermute(own, "cluster", pair_list(nclus, 0))
    second = lax.ppermute(own, "cluster", pair_list(nclus, 1))
    mapping = sds(order, tall, dtype=BF16)
    thin = sds(nmodes, order, dtype=BF16)
    lates = sds(nmodes, 4 * BLOCK, dtype=BF16)
    args = [meta, pltpu.with_memory_space_constraint(matrix, pltpu.HBM), rhs, basis,
            *inverses[1:], gathered, *got]
    others, *pairs, base, c_hi, c_lo = pl.pallas_call(
        setup_body,
        out_shape=[sds(2 * nmodes, width), mapping, mapping, thin, thin, lates, lates, full]
        + [sds(order, order, dtype=BF16)] * 2,
        in_specs=[SM, far] + [VM] * (len(args) - 2),
        out_specs=[VM] * 10,
        scratch_shapes=[pltpu.VMEM((order, order), F32), pltpu.SemaphoreType.DMA((order // ROWS,))],
        compiler_params=pltpu.CompilerParams(vmem_limit_bytes=16 << 20),
        cost_estimate=pl.CostEstimate(
            flops=100_000_000, bytes_accessed=1 << 22, transcendentals=0),
        name="setup",
    )(*args)
    c_pair = (c_hi, c_lo)
    b_pair, m_pair, l_pair = pairs[0:2], pairs[2:4], pairs[4:6]
    vee, image, *own_faces = call(
        first_apply_body, [full, full] + [block] * 4,
        [meta, base, *c_pair, *b_pair, own, others, first, second], smem_in=(0,))
    resid, eta = rhs, own

    resids, etas, scals = [resid], [eta], []
    along = None
    u_along = None
    for step in range(ITERS - 1):
        got = exchange(own_faces)
        if step == 0:
            main = call(sums_body, [sds(nmodes + PAD, width)],
                        [*m_pair, vee, image, resid, kappa, eta])[0]
            k_pair = call(maps_body, [mapping, mapping], [*c_pair, *b_pair],
                          flops=50_000_000)
        else:
            vee, resid, kappa, eta, *along, main = update(False)
            resids.append(resid)
            etas.append(eta)
        spread = call(coarse_late_body, [sds(nsub, nmodes + PAD, width)],
                      [main, *l_pair, *got])[0]
        gathered = gather(spread)
        qonce, qtwice, prod = call(
            faces_body, [full, full, full], [meta, image, *c_pair, *got],
            smem_in=(0,), flops=100_000_000)
        own, others, coarse = call(
            y_body, [sds(nmodes + PAD, width), sds(2 * nmodes, width), small],
            [*inverses, gathered])
        first, second = mirror(own)
        old = step > 0
        image_new, *u_next, scal, f0, f1, f2, f3 = call(
            make_image_body(old),
            [full] * (1 if old else 2) + [sds(PAD, width)] + [block] * 4,
            [meta, image, prod, *k_pair, own, others, first, second]
            + ([scals[-1], *u_along] if old else []), smem_in=(0,))
        own_faces, u_along = (f0, f1, f2, f3), u_next
        scals.append(scal)

        def update(last, scal=scal, vee=vee, qtwice=qtwice, own=own, others=others, first=first,
                   second=second, resid=resid, qonce=qonce, kappa=kappa, coarse=coarse, eta=eta,
                   image_new=image_new, along=along, old=old):
            outs = (
                [full, small, full, sds(nclus * nsub, 2, width)]
                if last
                else [full, full, small, small, full, full, small, small,
                      sds(nmodes + PAD, width)]
            )
            return call(
                make_update_body(old, last), outs,
                [scal, vee, qtwice, *b_pair, own, others, first, second, resid, qonce, kappa,
                 coarse, eta, image_new, *m_pair] + (list(along) if old else []),
                scratch=[pltpu.VMEM((order, width), F32), pltpu.VMEM((nmodes, width), F32)]
                if last else ())

        image = image_new

    resid, eta, q_along, main = update(True)
    resids.append(resid)
    etas.append(eta)
    got = exchange(own_faces)
    sums = call(fold_body, [sds(2, width)], [gather(main, ("cluster", "sub"))])[0]
    args = [meta, sums, *scals, *b_pair, *etas, *resids, q_along, image, *got]
    answer, resid = pl.pallas_call(
        finish_body,
        grid=(order // ROWS,),
        out_shape=[full, full],
        in_specs=[SM] + [VM] * (len(args) - 1),
        out_specs=[pl.BlockSpec((ROWS, width), lambda at: (at, 0))] * 2,
        compiler_params=pltpu.CompilerParams(vmem_limit_bytes=8 << 20),
        cost_estimate=pl.CostEstimate(
            flops=1_000_000, bytes_accessed=1 << 20, transcendentals=0),
        name="finish",
    )(*args)
    return (answer[None, None], resid[None, None])


def solution(mesh):
    return jax.shard_map(
        shards,
        mesh=mesh,
        in_specs=(
            P("cluster", "sub", None, None),
            P("cluster", "sub", None, None),
            P("cluster", "sub", None, None),
            P("cluster", "sub", None),
            P(),
            P(),
        ),
        out_specs=(P("cluster", "sub", None, None), P("cluster", "sub", None, None)),
        check_vma=False,
    )
```

```python
import jax
import jax.numpy as jnp
from jax import lax
from jax.experimental import pallas as pl
from jax.experimental.pallas import tpu as pltpu
from jax.sharding import PartitionSpec as P


BLOCK = 128
ITERS = 3
PAD = 8
ROWS = 256
TALL = 256
WIDE = 1024
F32 = jnp.float32
BF16 = jnp.bfloat16
VM = pl.BlockSpec(memory_space=pltpu.VMEM)
SM = pl.BlockSpec(memory_space=pltpu.SMEM)


def sds(*shape, dtype=F32):
    return jax.ShapeDtypeStruct(shape, dtype)


def call(body, outs, args, smem_in=(), smem_out=(), flops=1_000_000, mib=8,
         scratch=()):
    outs = list(outs)
    return pl.pallas_call(
        body,
        out_shape=outs,
        in_specs=[SM if at in smem_in else VM for at in range(len(args))],
        out_specs=[SM if at in smem_out else VM for at in range(len(outs))],
        scratch_shapes=list(scratch),
        compiler_params=pltpu.CompilerParams(vmem_limit_bytes=mib << 20),
        cost_estimate=pl.CostEstimate(
            flops=flops, bytes_accessed=1 << 20, transcendentals=0),
    )(*args)


def split(value):
    high = value.astype(BF16)
    return high, (value - high.astype(F32)).astype(BF16)


def dot(left, right):
    return jnp.dot(left, right, preferred_element_type=F32)


def dot3(left, right):
    return dot(left[0], right[0]) + (dot(left[0], right[1]) + dot(left[1], right[0]))


def dot_thin(left, right):
    high, low = left
    rows = high.shape[0]
    both = dot(jnp.concatenate([high, low], 0), right[0])
    return both[:rows] + (dot(high, right[1]) + both[rows:])


def dot6(left, right):
    return jnp.dot(left, right, precision=lax.Precision.HIGHEST, preferred_element_type=F32)


def pair_list(count, parity, wrap=False):
    pairs = []
    for low in range(parity, count - 1, 2):
        pairs += [(low, low + 1), (low + 1, low)]
    if wrap and parity == 1 and count > 2:
        pairs += [(count - 1, 0), (0, count - 1)]
    return pairs


def half(refs, rows):
    return refs[0][rows, :], refs[1][rows, :]


def start_body(face_in, edge_in, rhs_in, basis_in, inverse_in, *outs):
    *messages, meta, kappa, spread, rhs, basis, inverse_rows, face_block, edge_rows, sems = outs
    copies = [
        pltpu.make_async_copy(source, target, sems.at[at])
        for at, (source, target) in enumerate(
            ((face_in, face_block), (edge_in, edge_rows), (rhs_in, rhs), (basis_in, basis),
             (inverse_in, inverse_rows)))
    ]
    for copy in copies:
        copy.start()
    for copy in copies[:2]:
        copy.wait()
    nmodes = basis.shape[0]
    width = rhs.shape[1]
    clus, sub = lax.axis_index("cluster"), lax.axis_index("sub")
    link = 0
    for index, count, lower, upper, kind in (
        (sub, face_block.shape[2], 0, 1, 0),
        (clus, face_block.shape[0], 2, 3, 1),
    ):
        for parity in (0, 1):
            is_low = lax.rem(index + parity, 2) == 0
            partner = jnp.where(is_low, index + 1, index - 1)
            valid = (partner >= 0) & (partner < count)
            first = jnp.clip(jnp.minimum(index, partner), 0, count - 1)
            place = (clus, first) if kind == 0 else (first, sub)
            meta[link] = face_block[clus, jnp.where(is_low, upper, lower), sub] * BLOCK
            meta[4 + link] = jnp.where(valid, edge_rows[place[0], kind, place[1]], 0)
            link += 1
    for copy in copies[2:]:
        copy.wait()
    for at, message in enumerate(messages):
        start = pl.multiple_of(meta[at], BLOCK)
        message[:BLOCK] = rhs[pl.ds(start, BLOCK), :]
        message[BLOCK : BLOCK + nmodes, :BLOCK] = basis[:, pl.ds(start, BLOCK)]
        if width > BLOCK:
            message[BLOCK : BLOCK + nmodes, BLOCK:] = jnp.zeros((nmodes, width - BLOCK), F32)
        if at < 2:
            message[BLOCK + nmodes :] = inverse_rows[...]
    value = dot_thin(split(basis[...]), split(rhs[...]))
    kappa[...] = value
    for at in range(spread.shape[0]):
        spread[at] = value


def masks_of(starts, at, width):
    ids = lax.broadcasted_iota(jnp.int32, (BLOCK, width), 0)
    return (ids < starts[4 + at]).astype(F32)


def setup_body(starts, matrix, rhs, basis, i0, i1, gathered, g0, g1, g2, g3,
               others, b_hi, b_lo, m_hi, m_lo, l_hi, l_lo, base, c_hi, c_lo, held, sems):
    nmodes, order = basis.shape
    parts = [pl.ds(at * ROWS, ROWS) for at in range(order // ROWS)]
    copies = [
        pltpu.make_async_copy(matrix.at[part], held.at[part], sems.at[at])
        for at, part in enumerate(parts)
    ]
    for copy in copies:
        copy.start()
    skip = i0.shape[0] - nmodes
    others[:nmodes] = dot6(i0[skip:], gathered[...])
    others[nmodes:] = dot6(i1[skip:], gathered[...])
    width = rhs.shape[1]
    base[...] = rhs[...]
    m_hi[...], m_lo[...] = split(basis[...])
    b_hi[...] = jnp.zeros_like(b_hi)
    b_lo[...] = jnp.zeros_like(b_lo)
    own = basis[...].T
    b_hi[:, :nmodes], b_lo[:, :nmodes] = split(own)
    for at, got in enumerate((g0, g1, g2, g3)):
        start = pl.multiple_of(starts[at], BLOCK)
        rows = pl.ds(start, BLOCK)
        mask = 0.5 * masks_of(starts, at, width)
        base[rows, :] = base[rows, :] + mask * got[:BLOCK, :]
        theirs = got[BLOCK : BLOCK + nmodes, :BLOCK].T
        cols = slice((at + 1) * nmodes, (at + 2) * nmodes)
        b_hi[rows, cols], b_lo[rows, cols] = split(mask[:, :nmodes] * theirs)
        ids = lax.broadcasted_iota(jnp.int32, (nmodes, BLOCK), 1)
        weight = 0.5 * (ids < starts[4 + at]).astype(F32)
        cols = slice(at * BLOCK, (at + 1) * BLOCK)
        l_hi[:, cols], l_lo[:, cols] = split(weight * basis[:, pl.ds(start, BLOCK)])
    for part, copy in zip(parts, copies):
        copy.wait()

        @pl.loop(0, ROWS // 64)
        def _(at, part=part):
            rows = pl.ds(pl.multiple_of(part.start + at * 64, 64), 64)
            c_hi[rows, :], c_lo[rows, :] = split(held[rows, :])


def maps_body(c_hi, c_lo, b_hi, b_lo, k_hi, k_lo):
    k_hi[...], k_lo[...] = split(dot3((c_hi[...], c_lo[...]), (b_hi[...], b_lo[...])))


def copy_faces(starts, field, outs):
    for at, out in enumerate(outs):
        out[...] = field[pl.ds(pl.multiple_of(starts[at], BLOCK), BLOCK), :]


def first_y_body(inverse_rows, gathered, own):
    own[...] = dot6(inverse_rows[...], gathered[...])


def fold_body(everyone, out):
    total = everyone[0]
    for at in range(1, everyone.shape[0]):
        total = total + everyone[at]
    out[...] = total


def stacked(own, others, first, second):
    nmodes = others.shape[0] // 2
    return jnp.concatenate([own[:nmodes], others[...], first[:nmodes], second[:nmodes]], 0)


def first_apply_body(starts, base, c_hi, c_lo, b_hi, b_lo, own, others, first, second,
                     vee, image, *outs):
    ys = split(stacked(own, others, first, second))

    @pl.loop(0, base.shape[0] // ROWS)
    def _(at):
        rows = pl.ds(pl.multiple_of(at * ROWS, ROWS), ROWS)
        vee[rows, :] = base[rows, :] + dot3(half((b_hi, b_lo), rows), ys)

    image[...] = dot3((c_hi[...], c_lo[...]), split(vee[...]))

    copy_faces(starts, image, outs)


def column_sum(total):
    return jnp.sum(total, 0, keepdims=True)


def moment_rows(vee, image, resid, kappa, eta):
    width = resid.shape[1]

    def step(at, carry):
        rows = pl.ds(pl.multiple_of(at * BLOCK, BLOCK), BLOCK)
        value = resid[rows, :]
        squares = (value * value).reshape(-1, 8, width)
        curves = (vee[rows, :] * image[rows, :]).reshape(-1, 8, width)
        return carry[0] + jnp.sum(squares, 0), carry[1] + jnp.sum(curves, 0)

    zero = jnp.zeros((8, width), F32)
    rr, curve = lax.fori_loop(0, resid.shape[0] // BLOCK, step, (zero, zero))
    rz = column_sum(rr) + column_sum(kappa[...] * eta[...])
    curve = column_sum(curve)
    ids = lax.broadcasted_iota(jnp.int32, (PAD, width), 0)
    return jnp.where(ids == 0, rz, 0.0) + jnp.where(ids == 1, curve, 0.0)


def sums_body(m_hi, m_lo, vee, image, resid, kappa, eta, out):
    nmodes = kappa.shape[0]
    out[nmodes:] = moment_rows(vee, image, resid, kappa, eta)
    out[:nmodes] = dot_thin((m_hi[...], m_lo[...]), split(image[...]))


def coarse_late_body(main, l_hi, l_lo, g0, g1, g2, g3, spread):
    nmodes = l_hi.shape[0]
    total = main[:nmodes]
    for at, got in enumerate((g0, g1, g2, g3)):
        cols = slice(at * BLOCK, (at + 1) * BLOCK)
        total = total + dot_thin((l_hi[:, cols], l_lo[:, cols]), split(got[...]))
    for at in range(spread.shape[0]):
        for col in range(total.shape[1] // BLOCK):
            cols = slice(col * BLOCK, (col + 1) * BLOCK)
            spread[at, col * nmodes : (col + 1) * nmodes] = total[:, cols]
    packed = (total.shape[1] // BLOCK) * nmodes
    for at in range(spread.shape[0]):
        for col in range(total.shape[1] // BLOCK):
            cols = slice(col * BLOCK, (col + 1) * BLOCK)
            spread[at, packed + 2 * col : packed + 2 * (col + 1)] = main[nmodes : nmodes + 2, cols]


def faces_body(starts, image, c_hi, c_lo, g0, g1, g2, g3, qonce, qtwice, prod):
    width = image.shape[1]
    qonce[...] = image[...]
    qtwice[...] = image[...]
    for at, got in enumerate((g0, g1, g2, g3)):
        rows = pl.ds(pl.multiple_of(starts[at], BLOCK), BLOCK)
        mask = masks_of(starts, at, width)
        mine = image[rows, :]
        qonce[rows, :] = mine + (0.5 * mask) * got[...]
        qtwice[rows, :] = mine + mask * (got[...] + 0.25 * mine)
    prod[...] = dot3((c_hi[...], c_lo[...]), split(qtwice[...]))


def y_body(inverse_rows, i0, i1, gathered, own, others, coarse):
    count = gathered.shape[0]
    nmodes, width = coarse.shape
    groups = width // BLOCK

    def part(at, col):
        return gathered[at, col * nmodes : (col + 1) * nmodes]

    blocks = jnp.concatenate(
        [jnp.concatenate([part(at, col) for col in range(groups)], 1) for at in range(count)], 0)
    skip = i0.shape[0] - nmodes
    value = dot6(jnp.concatenate([inverse_rows[...], i0[skip:], i1[skip:]], 0), blocks)
    own[:nmodes] = value[:nmodes]
    others[...] = value[nmodes:]
    tail = gathered[0, groups * nmodes :]
    for at in range(1, count):
        tail = tail + gathered[at, groups * nmodes :]
    own[nmodes:] = jnp.zeros((PAD, width), F32)
    me = lax.axis_index("sub")
    for col in range(groups):
        cols = slice(col * BLOCK, (col + 1) * BLOCK)
        own[nmodes : nmodes + 2, cols] = tail[2 * col : 2 * (col + 1)]
        coarse[:, cols] = part(me, col)


def scalars(sums, rz_old, alpha_old):
    rz, curve = sums[0:1], sums[1:2]
    if rz_old is None:
        return rz / curve, None, rz
    beta = rz / rz_old
    return rz / (curve - beta * rz / alpha_old), beta, rz


def pack(alpha, beta, rz):
    ids = lax.broadcasted_iota(jnp.int32, (PAD, alpha.shape[1]), 0)
    out = jnp.where(ids == 0, alpha, 0.0) + jnp.where(ids == 2, rz, 0.0)
    return out if beta is None else out + jnp.where(ids == 1, beta, 0.0)


def make_image_body(has_old):
    def body(starts, image, prod, k_hi, k_lo, own, others, first, second, *rest):
        *rest, f0, f1, f2, f3 = rest
        nmodes = others.shape[0] // 2
        sums = own[nmodes:] + first[nmodes:] + second[nmodes:]
        if has_old:
            scal_old, along_old, image_new, scal = rest
            alpha, beta, rz = scalars(sums, scal_old[2:3], scal_old[0:1])
        else:
            image_new, along, scal = rest
            alpha, beta, rz = scalars(sums, None, None)
        scal[...] = pack(alpha, beta, rz)
        ys = split(stacked(own, others, first, second))

        @pl.loop(0, image.shape[0] // WIDE)
        def _(at):
            rows = pl.ds(pl.multiple_of(at * WIDE, WIDE), WIDE)
            value = prod[rows, :] + dot3(half((k_hi, k_lo), rows), ys)
            if has_old:
                value = value + beta * along_old[rows, :]
            if not has_old:
                along[rows, :] = value
            image_new[rows, :] = image[rows, :] - alpha * value

        copy_faces(starts, image_new, (f0, f1, f2, f3))

    return body


def make_update_body(has_old, last):
    def body(scal, vee, qtwice, b_hi, b_lo, own, others, first, second,
             resid, qonce, kappa, coarse, eta, image, m_hi, m_lo, *rest):
        if has_old:
            t_old, q_old, k_old, y_old = rest[:4]
            rest = rest[4:]
        if last:
            resid_new, eta_new, q_along, out, vee_new, kappa_new = rest
            t_along = k_along = y_along = None
        else:
            vee_new, resid_new, kappa_new, eta_new, t_along, q_along, k_along, y_along, out = rest
        alpha, beta = scal[0:1], scal[1:2]
        nmodes = kappa.shape[0]
        ys = split(stacked(own, others, first, second))

        def move(old, value, older):
            if has_old:
                value = value + beta * older
            return value, old - alpha * value

        @pl.loop(0, vee.shape[0] // WIDE)
        def _(at):
            rows = pl.ds(pl.multiple_of(at * WIDE, WIDE), WIDE)
            value = qtwice[rows, :] + dot3(half((b_hi, b_lo), rows), ys)
            value, vee_new[rows, :] = move(
                vee[rows, :], value, t_old[rows, :] if has_old else None)
            if not last:
                t_along[rows, :] = value
            q_along[rows, :], resid_new[rows, :] = move(
                resid[rows, :], qonce[rows, :], q_old[rows, :] if has_old else None)

        k_value, kappa_new[...] = move(kappa[...], coarse[...], k_old[...] if has_old else None)
        y_value, eta_new[...] = move(eta[...], own[:nmodes], y_old[...] if has_old else None)
        if not last:
            k_along[...], y_along[...] = k_value, y_value
        moments = moment_rows(vee_new, image, resid_new, kappa_new, eta_new)
        if last:
            for at in range(out.shape[0]):
                out[at] = moments[: out.shape[1]]
        else:
            out[:nmodes] = dot_thin((m_hi[...], m_lo[...]), split(image[...]))
            out[nmodes:] = moments

    return body


def finish_body(starts, sums, scal0, scal1, b_hi, b_lo, e0, e1, e2, r0, r1, r2, along, image,
                g0, g1, g2, g3, answer_out, resid_out, answer, resid, sems):
    nmodes = e0.shape[0]
    order, width = r0.shape
    alpha, beta, _ = scalars(sums[...], scal1[2:3], scal1[0:1])
    a1 = scal1[0:1] + beta * alpha
    a0 = scal0[0:1] + scal1[1:2] * a1
    chunks = [pl.ds(at * TALL, TALL) for at in range(order // TALL)]
    copies = []

    def send(source, target, rows):
        copy = pltpu.make_async_copy(source.at[rows], target.at[rows], sems.at[len(copies)])
        copy.start()
        copies.append(copy)

    ys = split(a0 * e0[...] + a1 * e1[...] + alpha * e2[...])
    for rows in chunks:
        part = dot3((b_hi[rows, :nmodes], b_lo[rows, :nmodes]), ys)
        answer[rows, :] = a0 * r0[rows, :] + a1 * r1[rows, :] + alpha * r2[rows, :] + part
        send(answer, answer_out, rows)
    for rows in chunks:
        resid[rows, :] = r2[rows, :] - alpha * (image[rows, :] + beta * along[rows, :])
    for which, got in enumerate((g0, g1, g2, g3)):
        part = pl.ds(pl.multiple_of(starts[which], BLOCK), BLOCK)
        mask = (0.5 * masks_of(starts, which, width)) * alpha
        resid[part, :] = resid[part, :] - mask * got[...]
    for rows in chunks:
        send(resid, resid_out, rows)
    for copy in copies:
        copy.wait()


def shards(compliance, loads, modes, coarse_inverse, face_block, edge_rows):
    matrix = compliance[0, 0]
    rhs = loads[0, 0]
    basis = modes[0, 0]
    inverse_rows = coarse_inverse[0]
    nmodes, order = basis.shape
    width = rhs.shape[1]
    coarse_all = inverse_rows.shape[1]
    nclus, nsub = lax.axis_size("cluster"), lax.axis_size("sub")
    full = sds(order, width)
    small = sds(nmodes, width)
    block = sds(BLOCK, width)
    tall = 5 * nmodes
    doubled = nclus == 4

    links = [("sub", pair_list(nsub, parity)) for parity in (0, 1)]
    links += [("cluster", pair_list(nclus, parity)) for parity in (0, 1)]

    def exchange(messages):
        got = [None] * 4
        for at in (1, 0, 3, 2):
            got[at] = lax.ppermute(messages[at], links[at][0], links[at][1])
        return got

    def gather(blocks, axis="sub"):
        return lax.all_to_all(blocks, axis, 0, 0, tiled=False)

    def mirror(ymom):
        first = lax.ppermute(ymom, "cluster", pair_list(nclus, 0))
        if doubled:
            sums = ymom[nmodes:] + first[nmodes:]
            both = jnp.concatenate([ymom[:nmodes], sums], 0)
            second = lax.ppermute(both, "cluster", pair_list(nclus, 1, True))
            return first, second
        mine = ymom[nmodes:]
        rest = lax.psum(mine, "cluster") - mine
        second = lax.ppermute(ymom[:nmodes], "cluster", pair_list(nclus, 1))
        return (
            jnp.concatenate([first[:nmodes], rest], 0),
            jnp.concatenate([second, jnp.zeros_like(rest)], 0),
        )

    extra = nmodes * coarse_all // width
    sizes = [BLOCK + nmodes + (extra if at < 2 else 0) for at in range(4)]
    far = pl.BlockSpec(memory_space=pltpu.HBM)
    *messages, meta, kappa, spread, rhs, basis, flat = pl.pallas_call(
        start_body,
        out_shape=[sds(size, width) for size in sizes]
        + [sds(8, dtype=jnp.int32), small, sds(nsub, nmodes, width), full,
           sds(nmodes, order), sds(extra, width)],
        in_specs=[far] * 5,
        out_specs=[VM] * 4 + [SM] + [VM] * 5,
        scratch_shapes=[
            pltpu.SMEM((nclus, 4, nsub), jnp.int32),
            pltpu.SMEM((nclus, 2, nsub), jnp.int32),
            pltpu.SemaphoreType.DMA((5,)),
        ],
        compiler_params=pltpu.CompilerParams(vmem_limit_bytes=16 << 20),
        name="start",
    )(*(pltpu.with_memory_space_constraint(each, pltpu.HBM) for each in (
        face_block.swapaxes(1, 2), edge_rows.swapaxes(1, 2), rhs, basis,
        inverse_rows.reshape(extra, width))))
    if coarse_all == width:
        inverse_rows = flat
    got = exchange(messages)
    gathered = gather(spread).reshape(nsub * nmodes, width)
    inverses = [inverse_rows, *got[:2]]
    if coarse_all != width:
        inverses[1:] = [each[BLOCK + nmodes :].reshape(nmodes, coarse_all) for each in got[:2]]
    own = call(first_y_body, [small], [inverse_rows, gathered])[0]
    first = lax.ppermute(own, "cluster", pair_list(nclus, 0))
    second = lax.ppermute(own, "cluster", pair_list(nclus, 1))
    mapping = sds(order, tall, dtype=BF16)
    thin = sds(nmodes, order, dtype=BF16)
    lates = sds(nmodes, 4 * BLOCK, dtype=BF16)
    args = [meta, pltpu.with_memory_space_constraint(matrix, pltpu.HBM), rhs, basis,
            *inverses[1:], gathered, *got]
    others, *pairs, base, c_hi, c_lo = pl.pallas_call(
        setup_body,
        out_shape=[sds(2 * nmodes, width), mapping, mapping, thin, thin, lates, lates, full]
        + [sds(order, order, dtype=BF16)] * 2,
        in_specs=[SM, far] + [VM] * (len(args) - 2),
        out_specs=[VM] * 10,
        scratch_shapes=[pltpu.VMEM((order, order), F32), pltpu.SemaphoreType.DMA((order // ROWS,))],
        compiler_params=pltpu.CompilerParams(vmem_limit_bytes=16 << 20),
        cost_estimate=pl.CostEstimate(
            flops=100_000_000, bytes_accessed=1 << 22, transcendentals=0),
        name="setup",
    )(*args)
    c_pair = (c_hi, c_lo)
    b_pair, m_pair, l_pair = pairs[0:2], pairs[2:4], pairs[4:6]
    vee, image, *own_faces = call(
        first_apply_body, [full, full] + [block] * 4,
        [meta, base, *c_pair, *b_pair, own, others, first, second], smem_in=(0,))
    resid, eta = rhs, own

    resids, etas, scals = [resid], [eta], []
    along = None
    u_along = None
    for step in range(ITERS - 1):
        got = exchange(own_faces)
        if step == 0:
            main = call(sums_body, [sds(nmodes + PAD, width)],
                        [*m_pair, vee, image, resid, kappa, eta])[0]
            k_pair = call(maps_body, [mapping, mapping], [*c_pair, *b_pair],
                          flops=50_000_000)
        else:
            vee, resid, kappa, eta, *along, main = update(False)
            resids.append(resid)
            etas.append(eta)
        spread = call(coarse_late_body, [sds(nsub, (nmodes + 2) * (width // BLOCK), BLOCK)],
                      [main, *l_pair, *got])[0]
        gathered = gather(spread)
        qonce, qtwice, prod = call(
            faces_body, [full, full, full], [meta, image, *c_pair, *got],
            smem_in=(0,), flops=100_000_000)
        own, others, coarse = call(
            y_body, [sds(nmodes + PAD, width), sds(2 * nmodes, width), small],
            [*inverses, gathered])
        first, second = mirror(own)
        old = step > 0
        image_new, *u_next, scal, f0, f1, f2, f3 = call(
            make_image_body(old),
            [full] * (1 if old else 2) + [sds(PAD, width)] + [block] * 4,
            [meta, image, prod, *k_pair, own, others, first, second]
            + ([scals[-1], *u_along] if old else []), smem_in=(0,))
        own_faces, u_along = (f0, f1, f2, f3), u_next
        scals.append(scal)

        def update(last, scal=scal, vee=vee, qtwice=qtwice, own=own, others=others, first=first,
                   second=second, resid=resid, qonce=qonce, kappa=kappa, coarse=coarse, eta=eta,
                   image_new=image_new, along=along, old=old):
            outs = (
                [full, small, full, sds(nclus * nsub, 2, width)]
                if last
                else [full, full, small, small, full, full, small, small,
                      sds(nmodes + PAD, width)]
            )
            return call(
                make_update_body(old, last), outs,
                [scal, vee, qtwice, *b_pair, own, others, first, second, resid, qonce, kappa,
                 coarse, eta, image_new, *m_pair] + (list(along) if old else []),
                scratch=[pltpu.VMEM((order, width), F32), pltpu.VMEM((nmodes, width), F32)]
                if last else ())

        image = image_new

    resid, eta, q_along, main = update(True)
    resids.append(resid)
    etas.append(eta)
    got = exchange(own_faces)
    sums = call(fold_body, [sds(2, width)], [gather(main, ("cluster", "sub"))])[0]
    args = [meta, sums, *scals, *b_pair, *etas, *resids, q_along, image, *got]
    answer, resid = pl.pallas_call(
        finish_body,
        out_shape=[full, full],
        in_specs=[SM] + [VM] * (len(args) - 1),
        out_specs=[far, far],
        scratch_shapes=[
            pltpu.VMEM((order, width), F32),
            pltpu.VMEM((order, width), F32),
            pltpu.SemaphoreType.DMA((2 * order // TALL,)),
        ],
        compiler_params=pltpu.CompilerParams(vmem_limit_bytes=8 << 20),
        cost_estimate=pl.CostEstimate(
            flops=1_000_000, bytes_accessed=1 << 20, transcendentals=0),
        name="finish",
    )(*args)
    return (answer[None, None], resid[None, None])


def solution(mesh):
    return jax.shard_map(
        shards,
        mesh=mesh,
        in_specs=(
            P("cluster", "sub", None, None),
            P("cluster", "sub", None, None),
            P("cluster", "sub", None, None),
            P("cluster", "sub", None),
            P(),
            P(),
        ),
        out_specs=(P("cluster", "sub", None, None), P("cluster", "sub", None, None)),
        check_vma=False,
    )
```

```python
import jax
import jax.numpy as jnp
from jax import lax
from jax.experimental import pallas as pl
from jax.experimental.pallas import tpu as pltpu
from jax.sharding import PartitionSpec as P


BLOCK = 128
ITERS = 3
PAD = 8
ROWS = 256
TALL = 256
WIDE = 1024
F32 = jnp.float32
BF16 = jnp.bfloat16
VM = pl.BlockSpec(memory_space=pltpu.VMEM)
SM = pl.BlockSpec(memory_space=pltpu.SMEM)


def sds(*shape, dtype=F32):
    return jax.ShapeDtypeStruct(shape, dtype)


def call(body, outs, args, smem_in=(), smem_out=(), flops=1_000_000, mib=8,
         scratch=()):
    outs = list(outs)
    return pl.pallas_call(
        body,
        out_shape=outs,
        in_specs=[SM if at in smem_in else VM for at in range(len(args))],
        out_specs=[SM if at in smem_out else VM for at in range(len(outs))],
        scratch_shapes=list(scratch),
        compiler_params=pltpu.CompilerParams(vmem_limit_bytes=mib << 20),
        cost_estimate=pl.CostEstimate(
            flops=flops, bytes_accessed=1 << 20, transcendentals=0),
    )(*args)


def split(value):
    high = value.astype(BF16)
    return high, (value - high.astype(F32)).astype(BF16)


def dot(left, right):
    return jnp.dot(left, right, preferred_element_type=F32)


def dot3(left, right):
    return dot(left[0], right[0]) + (dot(left[0], right[1]) + dot(left[1], right[0]))


def dot_thin(left, right):
    high, low = left
    rows = high.shape[0]
    both = dot(jnp.concatenate([high, low], 0), right[0])
    return both[:rows] + (dot(high, right[1]) + both[rows:])


def dot6(left, right):
    return jnp.dot(left, right, precision=lax.Precision.HIGHEST, preferred_element_type=F32)


def pair_list(count, parity, wrap=False):
    pairs = []
    for low in range(parity, count - 1, 2):
        pairs += [(low, low + 1), (low + 1, low)]
    if wrap and parity == 1 and count > 2:
        pairs += [(count - 1, 0), (0, count - 1)]
    return pairs


def half(refs, rows):
    return refs[0][rows, :], refs[1][rows, :]


def start_body(face_in, edge_in, rhs_in, basis_in, inverse_in, *outs):
    *messages, meta, kappa, spread, rhs, basis, inverse_rows, face_block, edge_rows, sems = outs
    copies = [
        pltpu.make_async_copy(source, target, sems.at[at])
        for at, (source, target) in enumerate(
            ((face_in, face_block), (edge_in, edge_rows), (rhs_in, rhs), (basis_in, basis),
             (inverse_in, inverse_rows)))
    ]
    for copy in copies:
        copy.start()
    for copy in copies[:2]:
        copy.wait()
    nmodes = basis.shape[0]
    width = rhs.shape[1]
    clus, sub = lax.axis_index("cluster"), lax.axis_index("sub")
    link = 0
    for index, count, lower, upper, kind in (
        (sub, face_block.shape[2], 0, 1, 0),
        (clus, face_block.shape[0], 2, 3, 1),
    ):
        for parity in (0, 1):
            is_low = lax.rem(index + parity, 2) == 0
            partner = jnp.where(is_low, index + 1, index - 1)
            valid = (partner >= 0) & (partner < count)
            first = jnp.clip(jnp.minimum(index, partner), 0, count - 1)
            place = (clus, first) if kind == 0 else (first, sub)
            meta[link] = face_block[clus, jnp.where(is_low, upper, lower), sub] * BLOCK
            meta[4 + link] = jnp.where(valid, edge_rows[place[0], kind, place[1]], 0)
            link += 1
    for copy in copies[2:]:
        copy.wait()
    for at, message in enumerate(messages):
        start = pl.multiple_of(meta[at], BLOCK)
        message[:BLOCK] = rhs[pl.ds(start, BLOCK), :]
        groups = width // BLOCK
        rows = nmodes // groups
        for col in range(groups):
            message[BLOCK : BLOCK + rows, col * BLOCK : (col + 1) * BLOCK] = basis[
                col * rows : (col + 1) * rows, pl.ds(start, BLOCK)]
        if at < 2:
            message[BLOCK + rows :] = inverse_rows[...]
    value = dot_thin(split(basis[...]), split(rhs[...]))
    kappa[...] = value
    for at in range(spread.shape[0]):
        spread[at] = value


def masks_of(starts, at, width):
    ids = lax.broadcasted_iota(jnp.int32, (BLOCK, width), 0)
    return (ids < starts[4 + at]).astype(F32)


def link_maps(got, mask, rows, at, nmodes, base, b_hi, b_lo):
    base[rows, :] = base[rows, :] + mask * got[:BLOCK, :]
    cols = slice((at + 1) * nmodes, (at + 2) * nmodes)
    b_hi[rows, cols], b_lo[rows, cols] = split(mask[:, :nmodes] * modes_of(got, nmodes).T)


def setup_body(starts, matrix, rhs, basis, i0, i1, gathered, g0, g1,
               others, b_hi, b_lo, m_hi, m_lo, l_hi, l_lo, base, c_hi, c_lo, held, sems):
    nmodes, order = basis.shape
    parts = [pl.ds(at * ROWS, ROWS) for at in range(order // ROWS)]
    copies = [
        pltpu.make_async_copy(matrix.at[part], held.at[part], sems.at[at])
        for at, part in enumerate(parts)
    ]
    for copy in copies:
        copy.start()
    skip = i0.shape[0] - nmodes
    others[:nmodes] = dot6(i0[skip:], gathered[...])
    others[nmodes:] = dot6(i1[skip:], gathered[...])
    width = rhs.shape[1]
    base[...] = rhs[...]
    m_hi[...], m_lo[...] = split(basis[...])
    b_hi[...] = jnp.zeros_like(b_hi)
    b_lo[...] = jnp.zeros_like(b_lo)
    own = basis[...].T
    b_hi[:, :nmodes], b_lo[:, :nmodes] = split(own)
    for at in range(4):
        start = pl.multiple_of(starts[at], BLOCK)
        rows = pl.ds(start, BLOCK)
        if at < 2:
            got = (g0, g1)[at]
            link_maps(got, 0.5 * masks_of(starts, at, width), rows, at, nmodes, base, b_hi, b_lo)
        ids = lax.broadcasted_iota(jnp.int32, (nmodes, BLOCK), 1)
        weight = 0.5 * (ids < starts[4 + at]).astype(F32)
        cols = slice(at * BLOCK, (at + 1) * BLOCK)
        l_hi[:, cols], l_lo[:, cols] = split(weight * basis[:, pl.ds(start, BLOCK)])
    for part, copy in zip(parts, copies):
        copy.wait()

        @pl.loop(0, ROWS // 64)
        def _(at, part=part):
            rows = pl.ds(pl.multiple_of(part.start + at * 64, 64), 64)
            c_hi[rows, :], c_lo[rows, :] = split(held[rows, :])


def maps_body(c_hi, c_lo, b_hi, b_lo, k_hi, k_lo):
    k_hi[...], k_lo[...] = split(dot3((c_hi[...], c_lo[...]), (b_hi[...], b_lo[...])))


def copy_faces(starts, field, outs):
    for at, out in enumerate(outs):
        out[...] = field[pl.ds(pl.multiple_of(starts[at], BLOCK), BLOCK), :]


def modes_of(got, nmodes):
    groups = got.shape[1] // BLOCK
    rows = nmodes // groups
    return jnp.concatenate(
        [got[BLOCK : BLOCK + rows, col * BLOCK : (col + 1) * BLOCK] for col in range(groups)], 0)


def first_y_body(inverse_rows, gathered, head0, head1, own, message0, message1):
    value = dot6(inverse_rows[...], gathered[...])
    own[...] = value
    for head, message in ((head0, message0), (head1, message1)):
        message[: head.shape[0]] = head[...]
        message[head.shape[0] :] = value


def fold_body(everyone, out):
    total = everyone[0]
    for at in range(1, everyone.shape[0]):
        total = total + everyone[at]
    out[...] = total


def stacked(own, others, first, second):
    nmodes = others.shape[0] // 2
    return jnp.concatenate([own[:nmodes], others[...], first[:nmodes], second[:nmodes]], 0)


def first_apply_body(starts, base, c_hi, c_lo, b_in_hi, b_in_lo, own, others, first, second,
                     vee, image, b_hi, b_lo, *outs):
    nmodes, width = own.shape
    vee[...] = base[...]
    b_hi[...], b_lo[...] = b_in_hi[...], b_in_lo[...]
    for at, got in ((2, first), (3, second)):
        rows = pl.ds(pl.multiple_of(starts[at], BLOCK), BLOCK)
        mask = 0.5 * masks_of(starts, at, width)
        link_maps(got, mask, rows, at, nmodes, vee, b_hi, b_lo)
    skip = first.shape[0] - nmodes
    ys = split(jnp.concatenate([own[...], others[...], first[skip:], second[skip:]], 0))

    @pl.loop(0, base.shape[0] // WIDE)
    def _(at):
        rows = pl.ds(pl.multiple_of(at * WIDE, WIDE), WIDE)
        vee[rows, :] = vee[rows, :] + dot3(half((b_hi, b_lo), rows), ys)

    image[...] = dot3((c_hi[...], c_lo[...]), split(vee[...]))
    copy_faces(starts, image, outs)


def column_sum(total):
    return jnp.sum(total, 0, keepdims=True)


def moment_rows(vee, image, resid, kappa, eta):
    width = resid.shape[1]

    def step(at, carry):
        rows = pl.ds(pl.multiple_of(at * BLOCK, BLOCK), BLOCK)
        value = resid[rows, :]
        squares = (value * value).reshape(-1, 8, width)
        curves = (vee[rows, :] * image[rows, :]).reshape(-1, 8, width)
        return carry[0] + jnp.sum(squares, 0), carry[1] + jnp.sum(curves, 0)

    zero = jnp.zeros((8, width), F32)
    rr, curve = lax.fori_loop(0, resid.shape[0] // BLOCK, step, (zero, zero))
    rz = column_sum(rr) + column_sum(kappa[...] * eta[...])
    curve = column_sum(curve)
    ids = lax.broadcasted_iota(jnp.int32, (PAD, width), 0)
    return jnp.where(ids == 0, rz, 0.0) + jnp.where(ids == 1, curve, 0.0)


def sums_body(m_hi, m_lo, vee, image, resid, kappa, eta, out):
    nmodes = kappa.shape[0]
    out[nmodes:] = moment_rows(vee, image, resid, kappa, eta)
    out[:nmodes] = dot_thin((m_hi[...], m_lo[...]), split(image[...]))


def coarse_late_body(main, l_hi, l_lo, g0, g1, g2, g3, spread):
    nmodes = l_hi.shape[0]
    total = main[:nmodes]
    for at, got in enumerate((g0, g1, g2, g3)):
        cols = slice(at * BLOCK, (at + 1) * BLOCK)
        total = total + dot_thin((l_hi[:, cols], l_lo[:, cols]), split(got[...]))
    for at in range(spread.shape[0]):
        for col in range(total.shape[1] // BLOCK):
            cols = slice(col * BLOCK, (col + 1) * BLOCK)
            spread[at, col * nmodes : (col + 1) * nmodes] = total[:, cols]
    packed = (total.shape[1] // BLOCK) * nmodes
    for at in range(spread.shape[0]):
        for col in range(total.shape[1] // BLOCK):
            cols = slice(col * BLOCK, (col + 1) * BLOCK)
            spread[at, packed + 2 * col : packed + 2 * (col + 1)] = main[nmodes : nmodes + 2, cols]


def faces_body(starts, image, c_hi, c_lo, g0, g1, g2, g3, qonce, qtwice, prod):
    width = image.shape[1]
    qonce[...] = image[...]
    qtwice[...] = image[...]
    for at, got in enumerate((g0, g1, g2, g3)):
        rows = pl.ds(pl.multiple_of(starts[at], BLOCK), BLOCK)
        mask = masks_of(starts, at, width)
        mine = image[rows, :]
        qonce[rows, :] = mine + (0.5 * mask) * got[...]
        qtwice[rows, :] = mine + mask * (got[...] + 0.25 * mine)
    prod[...] = dot3((c_hi[...], c_lo[...]), split(qtwice[...]))


def y_body(inverse_rows, i0, i1, gathered, own, others, coarse):
    count = gathered.shape[0]
    nmodes, width = coarse.shape
    groups = width // BLOCK

    def part(at, col):
        return gathered[at, col * nmodes : (col + 1) * nmodes]

    blocks = jnp.concatenate(
        [jnp.concatenate([part(at, col) for col in range(groups)], 1) for at in range(count)], 0)
    skip = i0.shape[0] - nmodes
    value = dot6(jnp.concatenate([inverse_rows[...], i0[skip:], i1[skip:]], 0), blocks)
    own[:nmodes] = value[:nmodes]
    others[...] = value[nmodes:]
    tail = gathered[0, groups * nmodes :]
    for at in range(1, count):
        tail = tail + gathered[at, groups * nmodes :]
    own[nmodes:] = jnp.zeros((PAD, width), F32)
    me = lax.axis_index("sub")
    for col in range(groups):
        cols = slice(col * BLOCK, (col + 1) * BLOCK)
        own[nmodes : nmodes + 2, cols] = tail[2 * col : 2 * (col + 1)]
        coarse[:, cols] = part(me, col)


def scalars(sums, rz_old, alpha_old):
    rz, curve = sums[0:1], sums[1:2]
    if rz_old is None:
        return rz / curve, None, rz
    beta = rz / rz_old
    return rz / (curve - beta * rz / alpha_old), beta, rz


def pack(alpha, beta, rz):
    ids = lax.broadcasted_iota(jnp.int32, (PAD, alpha.shape[1]), 0)
    out = jnp.where(ids == 0, alpha, 0.0) + jnp.where(ids == 2, rz, 0.0)
    return out if beta is None else out + jnp.where(ids == 1, beta, 0.0)


def make_image_body(has_old):
    def body(starts, image, prod, k_hi, k_lo, own, others, first, second, *rest):
        *rest, f0, f1, f2, f3 = rest
        nmodes = others.shape[0] // 2
        sums = own[nmodes:] + first[nmodes:] + second[nmodes:]
        if has_old:
            scal_old, along_old, image_new, scal = rest
            alpha, beta, rz = scalars(sums, scal_old[2:3], scal_old[0:1])
        else:
            image_new, along, scal = rest
            alpha, beta, rz = scalars(sums, None, None)
        scal[...] = pack(alpha, beta, rz)
        ys = split(stacked(own, others, first, second))

        @pl.loop(0, image.shape[0] // WIDE)
        def _(at):
            rows = pl.ds(pl.multiple_of(at * WIDE, WIDE), WIDE)
            value = prod[rows, :] + dot3(half((k_hi, k_lo), rows), ys)
            if has_old:
                value = value + beta * along_old[rows, :]
            if not has_old:
                along[rows, :] = value
            image_new[rows, :] = image[rows, :] - alpha * value

        copy_faces(starts, image_new, (f0, f1, f2, f3))

    return body


def make_update_body(has_old, last):
    def body(scal, vee, qtwice, b_hi, b_lo, own, others, first, second,
             resid, qonce, kappa, coarse, eta, image, m_hi, m_lo, *rest):
        if has_old:
            t_old, q_old, k_old, y_old = rest[:4]
            rest = rest[4:]
        if last:
            resid_new, eta_new, q_along, out, vee_new, kappa_new = rest
            t_along = k_along = y_along = None
        else:
            vee_new, resid_new, kappa_new, eta_new, t_along, q_along, k_along, y_along, out = rest
        alpha, beta = scal[0:1], scal[1:2]
        nmodes = kappa.shape[0]
        ys = split(stacked(own, others, first, second))

        def move(old, value, older):
            if has_old:
                value = value + beta * older
            return value, old - alpha * value

        @pl.loop(0, vee.shape[0] // WIDE)
        def _(at):
            rows = pl.ds(pl.multiple_of(at * WIDE, WIDE), WIDE)
            value = qtwice[rows, :] + dot3(half((b_hi, b_lo), rows), ys)
            value, vee_new[rows, :] = move(
                vee[rows, :], value, t_old[rows, :] if has_old else None)
            if not last:
                t_along[rows, :] = value
            q_along[rows, :], resid_new[rows, :] = move(
                resid[rows, :], qonce[rows, :], q_old[rows, :] if has_old else None)

        k_value, kappa_new[...] = move(kappa[...], coarse[...], k_old[...] if has_old else None)
        y_value, eta_new[...] = move(eta[...], own[:nmodes], y_old[...] if has_old else None)
        if not last:
            k_along[...], y_along[...] = k_value, y_value
        moments = moment_rows(vee_new, image, resid_new, kappa_new, eta_new)
        if last:
            for at in range(out.shape[0]):
                out[at] = moments[: out.shape[1]]
        else:
            out[:nmodes] = dot_thin((m_hi[...], m_lo[...]), split(image[...]))
            out[nmodes:] = moments

    return body


def finish_body(starts, sums, scal0, scal1, b_hi, b_lo, e0, e1, e2, r0, r1, r2, along, image,
                g0, g1, g2, g3, answer_out, resid_out, answer, resid, sems):
    nmodes = e0.shape[0]
    order, width = r0.shape
    alpha, beta, _ = scalars(sums[...], scal1[2:3], scal1[0:1])
    a1 = scal1[0:1] + beta * alpha
    a0 = scal0[0:1] + scal1[1:2] * a1
    chunks = [pl.ds(at * TALL, TALL) for at in range(order // TALL)]
    copies = []

    def send(source, target, rows):
        copy = pltpu.make_async_copy(source.at[rows], target.at[rows], sems.at[len(copies)])
        copy.start()
        copies.append(copy)

    ys = split(a0 * e0[...] + a1 * e1[...] + alpha * e2[...])
    for rows in chunks:
        part = dot3((b_hi[rows, :nmodes], b_lo[rows, :nmodes]), ys)
        answer[rows, :] = a0 * r0[rows, :] + a1 * r1[rows, :] + alpha * r2[rows, :] + part
        send(answer, answer_out, rows)
    for rows in chunks:
        resid[rows, :] = r2[rows, :] - alpha * (image[rows, :] + beta * along[rows, :])
    for which, got in enumerate((g0, g1, g2, g3)):
        part = pl.ds(pl.multiple_of(starts[which], BLOCK), BLOCK)
        mask = (0.5 * masks_of(starts, which, width)) * alpha
        resid[part, :] = resid[part, :] - mask * got[...]
    for rows in chunks:
        send(resid, resid_out, rows)
    for copy in copies:
        copy.wait()


def shards(compliance, loads, modes, coarse_inverse, face_block, edge_rows):
    matrix = compliance[0, 0]
    rhs = loads[0, 0]
    basis = modes[0, 0]
    inverse_rows = coarse_inverse[0]
    nmodes, order = basis.shape
    width = rhs.shape[1]
    coarse_all = inverse_rows.shape[1]
    nclus, nsub = lax.axis_size("cluster"), lax.axis_size("sub")
    full = sds(order, width)
    small = sds(nmodes, width)
    block = sds(BLOCK, width)
    tall = 5 * nmodes
    doubled = nclus == 4

    links = [("sub", pair_list(nsub, parity)) for parity in (0, 1)]
    links += [("cluster", pair_list(nclus, parity)) for parity in (0, 1)]

    def exchange(messages):
        got = [None] * 4
        for at in (1, 0, 3, 2):
            got[at] = lax.ppermute(messages[at], links[at][0], links[at][1])
        return got

    def gather(blocks, axis="sub"):
        return lax.all_to_all(blocks, axis, 0, 0, tiled=False)

    def mirror(ymom):
        first = lax.ppermute(ymom, "cluster", pair_list(nclus, 0))
        if doubled:
            sums = ymom[nmodes:] + first[nmodes:]
            both = jnp.concatenate([ymom[:nmodes], sums], 0)
            second = lax.ppermute(both, "cluster", pair_list(nclus, 1, True))
            return first, second
        mine = ymom[nmodes:]
        rest = lax.psum(mine, "cluster") - mine
        second = lax.ppermute(ymom[:nmodes], "cluster", pair_list(nclus, 1))
        return (
            jnp.concatenate([first[:nmodes], rest], 0),
            jnp.concatenate([second, jnp.zeros_like(rest)], 0),
        )

    extra = nmodes * coarse_all // width
    head = BLOCK + nmodes * BLOCK // width
    sizes = [head + (extra if at < 2 else 0) for at in range(4)]
    far = pl.BlockSpec(memory_space=pltpu.HBM)
    *messages, meta, kappa, spread, rhs, basis, flat = pl.pallas_call(
        start_body,
        out_shape=[sds(size, width) for size in sizes]
        + [sds(8, dtype=jnp.int32), small, sds(nsub, nmodes, width), full,
           sds(nmodes, order), sds(extra, width)],
        in_specs=[far] * 5,
        out_specs=[VM] * 4 + [SM] + [VM] * 5,
        scratch_shapes=[
            pltpu.SMEM((nclus, 4, nsub), jnp.int32),
            pltpu.SMEM((nclus, 2, nsub), jnp.int32),
            pltpu.SemaphoreType.DMA((5,)),
        ],
        compiler_params=pltpu.CompilerParams(vmem_limit_bytes=16 << 20),
        name="start",
    )(*(pltpu.with_memory_space_constraint(each, pltpu.HBM) for each in (
        face_block.swapaxes(1, 2), edge_rows.swapaxes(1, 2), rhs, basis,
        inverse_rows.reshape(extra, width))))
    if coarse_all == width:
        inverse_rows = flat
    got = [None] * 2
    for at in (1, 0):
        got[at] = lax.ppermute(messages[at], links[at][0], links[at][1])
    gathered = gather(spread).reshape(nsub * nmodes, width)
    inverses = [inverse_rows, *got]
    if coarse_all != width:
        inverses[1:] = [each[head:].reshape(nmodes, coarse_all) for each in got]
    joined = sds(head + nmodes, width)
    own, *tails = call(
        first_y_body, [small, joined, joined], [inverse_rows, gathered, *messages[2:]])
    second = lax.ppermute(tails[1], "cluster", pair_list(nclus, 1))
    first = lax.ppermute(tails[0], "cluster", pair_list(nclus, 0))
    mapping = sds(order, tall, dtype=BF16)
    thin = sds(nmodes, order, dtype=BF16)
    lates = sds(nmodes, 4 * BLOCK, dtype=BF16)
    args = [meta, pltpu.with_memory_space_constraint(matrix, pltpu.HBM), rhs, basis,
            *inverses[1:], gathered, *got]
    others, *pairs, base, c_hi, c_lo = pl.pallas_call(
        setup_body,
        out_shape=[sds(2 * nmodes, width), mapping, mapping, thin, thin, lates, lates, full]
        + [sds(order, order, dtype=BF16)] * 2,
        in_specs=[SM, far] + [VM] * (len(args) - 2),
        out_specs=[VM] * 10,
        scratch_shapes=[pltpu.VMEM((order, order), F32), pltpu.SemaphoreType.DMA((order // ROWS,))],
        compiler_params=pltpu.CompilerParams(vmem_limit_bytes=16 << 20),
        cost_estimate=pl.CostEstimate(
            flops=100_000_000, bytes_accessed=1 << 22, transcendentals=0),
        name="setup",
    )(*args)
    c_pair = (c_hi, c_lo)
    b_pair, m_pair, l_pair = pairs[0:2], pairs[2:4], pairs[4:6]
    vee, image, *b_pair, f0, f1, f2, f3 = call(
        first_apply_body, [full, full, mapping, mapping] + [block] * 4,
        [meta, base, *c_pair, *b_pair, own, others, first, second], smem_in=(0,))
    own_faces = (f0, f1, f2, f3)
    resid, eta = rhs, own

    resids, etas, scals = [resid], [eta], []
    along = None
    u_along = None
    for step in range(ITERS - 1):
        got = exchange(own_faces)
        if step == 0:
            main = call(sums_body, [sds(nmodes + PAD, width)],
                        [*m_pair, vee, image, resid, kappa, eta])[0]
            k_pair = call(maps_body, [mapping, mapping], [*c_pair, *b_pair],
                          flops=50_000_000)
        else:
            vee, resid, kappa, eta, *along, main = update(False)
            resids.append(resid)
            etas.append(eta)
        spread = call(coarse_late_body, [sds(nsub, (nmodes + 2) * (width // BLOCK), BLOCK)],
                      [main, *l_pair, *got])[0]
        gathered = gather(spread)
        qonce, qtwice, prod = call(
            faces_body, [full, full, full], [meta, image, *c_pair, *got],
            smem_in=(0,), flops=100_000_000)
        own, others, coarse = call(
            y_body, [sds(nmodes + PAD, width), sds(2 * nmodes, width), small],
            [*inverses, gathered])
        first, second = mirror(own)
        old = step > 0
        image_new, *u_next, scal, f0, f1, f2, f3 = call(
            make_image_body(old),
            [full] * (1 if old else 2) + [sds(PAD, width)] + [block] * 4,
            [meta, image, prod, *k_pair, own, others, first, second]
            + ([scals[-1], *u_along] if old else []), smem_in=(0,))
        own_faces, u_along = (f0, f1, f2, f3), u_next
        scals.append(scal)

        def update(last, scal=scal, vee=vee, qtwice=qtwice, own=own, others=others, first=first,
                   second=second, resid=resid, qonce=qonce, kappa=kappa, coarse=coarse, eta=eta,
                   image_new=image_new, along=along, old=old):
            outs = (
                [full, small, full, sds(nclus * nsub, 2, width)]
                if last
                else [full, full, small, small, full, full, small, small,
                      sds(nmodes + PAD, width)]
            )
            return call(
                make_update_body(old, last), outs,
                [scal, vee, qtwice, *b_pair, own, others, first, second, resid, qonce, kappa,
                 coarse, eta, image_new, *m_pair] + (list(along) if old else []),
                scratch=[pltpu.VMEM((order, width), F32), pltpu.VMEM((nmodes, width), F32)]
                if last else ())

        image = image_new

    resid, eta, q_along, main = update(True)
    resids.append(resid)
    etas.append(eta)
    got = exchange(own_faces)
    sums = call(fold_body, [sds(2, width)], [gather(main, ("cluster", "sub"))])[0]
    args = [meta, sums, *scals, *b_pair, *etas, *resids, q_along, image, *got]
    answer, resid = pl.pallas_call(
        finish_body,
        out_shape=[full, full],
        in_specs=[SM] + [VM] * (len(args) - 1),
        out_specs=[far, far],
        scratch_shapes=[
            pltpu.VMEM((order, width), F32),
            pltpu.VMEM((order, width), F32),
            pltpu.SemaphoreType.DMA((2 * order // TALL,)),
        ],
        compiler_params=pltpu.CompilerParams(vmem_limit_bytes=8 << 20),
        cost_estimate=pl.CostEstimate(
            flops=1_000_000, bytes_accessed=1 << 20, transcendentals=0),
        name="finish",
    )(*args)
    return (answer[None, None], resid[None, None])


def solution(mesh):
    return jax.shard_map(
        shards,
        mesh=mesh,
        in_specs=(
            P("cluster", "sub", None, None),
            P("cluster", "sub", None, None),
            P("cluster", "sub", None, None),
            P("cluster", "sub", None),
            P(),
            P(),
        ),
        out_specs=(P("cluster", "sub", None, None), P("cluster", "sub", None, None)),
        check_vma=False,
    )
```

```python
import jax
import jax.numpy as jnp
from jax import lax
from jax.experimental import pallas as pl
from jax.experimental.pallas import tpu as pltpu
from jax.sharding import PartitionSpec as P


BLOCK = 128
ITERS = 3
PAD = 8
ROWS = 256
TALL = 256
WIDE = 1024
F32 = jnp.float32
BF16 = jnp.bfloat16
VM = pl.BlockSpec(memory_space=pltpu.VMEM)
SM = pl.BlockSpec(memory_space=pltpu.SMEM)


def sds(*shape, dtype=F32):
    return jax.ShapeDtypeStruct(shape, dtype)


def call(body, outs, args, smem_in=(), smem_out=(), flops=1_000_000, mib=8,
         scratch=()):
    outs = list(outs)
    return pl.pallas_call(
        body,
        out_shape=outs,
        in_specs=[SM if at in smem_in else VM for at in range(len(args))],
        out_specs=[SM if at in smem_out else VM for at in range(len(outs))],
        scratch_shapes=list(scratch),
        compiler_params=pltpu.CompilerParams(vmem_limit_bytes=mib << 20),
        cost_estimate=pl.CostEstimate(
            flops=flops, bytes_accessed=1 << 20, transcendentals=0),
    )(*args)


def split(value):
    high = value.astype(BF16)
    return high, (value - high.astype(F32)).astype(BF16)


def dot(left, right):
    return jnp.dot(left, right, preferred_element_type=F32)


def dot3(left, right):
    return dot(left[0], right[0]) + (dot(left[0], right[1]) + dot(left[1], right[0]))


def dot_thin(left, right):
    high, low = left
    rows = high.shape[0]
    both = dot(jnp.concatenate([high, low], 0), right[0])
    return both[:rows] + (dot(high, right[1]) + both[rows:])


def dot6(left, right):
    return jnp.dot(left, right, precision=lax.Precision.HIGHEST, preferred_element_type=F32)


def pair_list(count, parity, wrap=False):
    pairs = []
    for low in range(parity, count - 1, 2):
        pairs += [(low, low + 1), (low + 1, low)]
    if wrap and parity == 1 and count > 2:
        pairs += [(count - 1, 0), (0, count - 1)]
    return pairs


def half(refs, rows):
    return refs[0][rows, :], refs[1][rows, :]


def start_body(face_in, edge_in, rhs_in, basis_in, inverse_in, *outs):
    *messages, meta, kappa, spread, rhs, basis, inverse_rows, face_block, edge_rows, sems = outs
    copies = [
        pltpu.make_async_copy(source, target, sems.at[at])
        for at, (source, target) in enumerate(
            ((face_in, face_block), (edge_in, edge_rows), (rhs_in, rhs), (basis_in, basis),
             (inverse_in, inverse_rows)))
    ]
    for copy in copies:
        copy.start()
    for copy in copies[:2]:
        copy.wait()
    nmodes = basis.shape[0]
    width = rhs.shape[1]
    clus, sub = lax.axis_index("cluster"), lax.axis_index("sub")
    link = 0
    for index, count, lower, upper, kind in (
        (sub, face_block.shape[2], 0, 1, 0),
        (clus, face_block.shape[0], 2, 3, 1),
    ):
        for parity in (0, 1):
            is_low = lax.rem(index + parity, 2) == 0
            partner = jnp.where(is_low, index + 1, index - 1)
            valid = (partner >= 0) & (partner < count)
            first = jnp.clip(jnp.minimum(index, partner), 0, count - 1)
            place = (clus, first) if kind == 0 else (first, sub)
            meta[link] = face_block[clus, jnp.where(is_low, upper, lower), sub] * BLOCK
            meta[4 + link] = jnp.where(valid, edge_rows[place[0], kind, place[1]], 0)
            link += 1
    for copy in copies[2:]:
        copy.wait()
    for at, message in enumerate(messages):
        start = pl.multiple_of(meta[at], BLOCK)
        message[:BLOCK] = rhs[pl.ds(start, BLOCK), :]
        groups = width // BLOCK
        rows = nmodes // groups
        for col in range(groups):
            message[BLOCK : BLOCK + rows, col * BLOCK : (col + 1) * BLOCK] = basis[
                col * rows : (col + 1) * rows, pl.ds(start, BLOCK)]
        if at < 2:
            message[BLOCK + rows :] = inverse_rows[...]
    value = dot_thin(split(basis[...]), split(rhs[...]))
    kappa[...] = value
    for at in range(spread.shape[0]):
        spread[at] = value


def masks_of(starts, at, width):
    ids = lax.broadcasted_iota(jnp.int32, (BLOCK, width), 0)
    return (ids < starts[4 + at]).astype(F32)


def link_maps(got, mask, rows, at, nmodes, base, b_hi, b_lo):
    base[rows, :] = base[rows, :] + mask * got[:BLOCK, :]
    cols = slice((at + 1) * nmodes, (at + 2) * nmodes)
    b_hi[rows, cols], b_lo[rows, cols] = split(mask[:, :nmodes] * modes_of(got, nmodes).T)


def setup_body(starts, matrix, rhs, basis, i0, i1, gathered, g0, g1,
               others, b_hi, b_lo, m_hi, m_lo, l_hi, l_lo, base, c_hi, c_lo, held, sems):
    nmodes, order = basis.shape
    parts = [pl.ds(at * ROWS, ROWS) for at in range(order // ROWS)]
    copies = [
        pltpu.make_async_copy(matrix.at[part], held.at[part], sems.at[at])
        for at, part in enumerate(parts)
    ]
    for copy in copies:
        copy.start()
    skip = i0.shape[0] - nmodes
    others[:nmodes] = dot6(i0[skip:], gathered[...])
    others[nmodes:] = dot6(i1[skip:], gathered[...])
    width = rhs.shape[1]
    base[...] = rhs[...]
    m_hi[...], m_lo[...] = split(basis[...])
    b_hi[...] = jnp.zeros_like(b_hi)
    b_lo[...] = jnp.zeros_like(b_lo)
    own = basis[...].T
    b_hi[:, :nmodes], b_lo[:, :nmodes] = split(own)
    for at in range(4):
        start = pl.multiple_of(starts[at], BLOCK)
        rows = pl.ds(start, BLOCK)
        if at < 2:
            got = (g0, g1)[at]
            link_maps(got, 0.5 * masks_of(starts, at, width), rows, at, nmodes, base, b_hi, b_lo)
        ids = lax.broadcasted_iota(jnp.int32, (nmodes, BLOCK), 1)
        weight = 0.5 * (ids < starts[4 + at]).astype(F32)
        cols = slice(at * BLOCK, (at + 1) * BLOCK)
        l_hi[:, cols], l_lo[:, cols] = split(weight * basis[:, pl.ds(start, BLOCK)])
    for part, copy in zip(parts, copies):
        copy.wait()

        @pl.loop(0, ROWS // 64)
        def _(at, part=part):
            rows = pl.ds(pl.multiple_of(part.start + at * 64, 64), 64)
            c_hi[rows, :], c_lo[rows, :] = split(held[rows, :])


def maps_body(c_hi, c_lo, b_hi, b_lo, k_hi, k_lo):
    k_hi[...], k_lo[...] = split(dot3((c_hi[...], c_lo[...]), (b_hi[...], b_lo[...])))


def copy_faces(starts, field, outs):
    for at, out in enumerate(outs):
        out[...] = field[pl.ds(pl.multiple_of(starts[at], BLOCK), BLOCK), :]


def modes_of(got, nmodes):
    groups = got.shape[1] // BLOCK
    rows = nmodes // groups
    return jnp.concatenate(
        [got[BLOCK : BLOCK + rows, col * BLOCK : (col + 1) * BLOCK] for col in range(groups)], 0)


def first_y_body(inverse_rows, gathered, head0, head1, own, message0, message1):
    value = dot6(inverse_rows[...], gathered[...])
    own[...] = value
    for head, message in ((head0, message0), (head1, message1)):
        message[: head.shape[0]] = head[...]
        message[head.shape[0] :] = value


def fold_body(everyone, out):
    total = everyone[0]
    for at in range(1, everyone.shape[0]):
        total = total + everyone[at]
    out[...] = total


def stacked(own, others, first, second):
    nmodes = others.shape[0] // 2
    return jnp.concatenate([own[:nmodes], others[...], first[:nmodes], second[:nmodes]], 0)


def first_apply_body(starts, base, c_hi, c_lo, b_in_hi, b_in_lo, own, others, first, second,
                     vee, image, b_hi, b_lo, *outs):
    nmodes, width = own.shape
    vee[...] = base[...]
    b_hi[...], b_lo[...] = b_in_hi[...], b_in_lo[...]
    for at, got in ((2, first), (3, second)):
        rows = pl.ds(pl.multiple_of(starts[at], BLOCK), BLOCK)
        mask = 0.5 * masks_of(starts, at, width)
        link_maps(got, mask, rows, at, nmodes, vee, b_hi, b_lo)
    skip = first.shape[0] - nmodes
    ys = split(jnp.concatenate([own[...], others[...], first[skip:], second[skip:]], 0))

    @pl.loop(0, base.shape[0] // WIDE)
    def _(at):
        rows = pl.ds(pl.multiple_of(at * WIDE, WIDE), WIDE)
        vee[rows, :] = vee[rows, :] + dot3(half((b_hi, b_lo), rows), ys)

    image[...] = dot3((c_hi[...], c_lo[...]), split(vee[...]))
    copy_faces(starts, image, outs)


def column_sum(total):
    return jnp.sum(total, 0, keepdims=True)


def moment_rows(vee, image, resid, kappa, eta):
    width = resid.shape[1]

    def step(at, carry):
        rows = pl.ds(pl.multiple_of(at * BLOCK, BLOCK), BLOCK)
        value = resid[rows, :]
        squares = (value * value).reshape(-1, 8, width)
        curves = (vee[rows, :] * image[rows, :]).reshape(-1, 8, width)
        return carry[0] + jnp.sum(squares, 0), carry[1] + jnp.sum(curves, 0)

    zero = jnp.zeros((8, width), F32)
    rr, curve = lax.fori_loop(0, resid.shape[0] // BLOCK, step, (zero, zero))
    rz = column_sum(rr) + column_sum(kappa[...] * eta[...])
    curve = column_sum(curve)
    ids = lax.broadcasted_iota(jnp.int32, (PAD, width), 0)
    return jnp.where(ids == 0, rz, 0.0) + jnp.where(ids == 1, curve, 0.0)


def sums_body(m_hi, m_lo, vee, image, resid, kappa, eta, out):
    nmodes = kappa.shape[0]
    out[nmodes:] = moment_rows(vee, image, resid, kappa, eta)
    out[:nmodes] = dot_thin((m_hi[...], m_lo[...]), split(image[...]))


def coarse_late_body(main, l_hi, l_lo, g0, g1, g2, g3, spread):
    nmodes = l_hi.shape[0]
    total = main[:nmodes]
    for at, got in enumerate((g0, g1, g2, g3)):
        cols = slice(at * BLOCK, (at + 1) * BLOCK)
        total = total + dot_thin((l_hi[:, cols], l_lo[:, cols]), split(got[...]))
    for at in range(spread.shape[0]):
        for col in range(total.shape[1] // BLOCK):
            cols = slice(col * BLOCK, (col + 1) * BLOCK)
            spread[at, col * nmodes : (col + 1) * nmodes] = total[:, cols]
    packed = (total.shape[1] // BLOCK) * nmodes
    for at in range(spread.shape[0]):
        for col in range(total.shape[1] // BLOCK):
            cols = slice(col * BLOCK, (col + 1) * BLOCK)
            spread[at, packed + 2 * col : packed + 2 * (col + 1)] = main[nmodes : nmodes + 2, cols]


def faces_body(starts, image, c_hi, c_lo, g0, g1, g2, g3, qonce, qtwice, prod):
    width = image.shape[1]
    qonce[...] = image[...]
    qtwice[...] = image[...]
    for at, got in enumerate((g0, g1, g2, g3)):
        rows = pl.ds(pl.multiple_of(starts[at], BLOCK), BLOCK)
        mask = masks_of(starts, at, width)
        mine = image[rows, :]
        qonce[rows, :] = mine + (0.5 * mask) * got[...]
        qtwice[rows, :] = mine + mask * (got[...] + 0.25 * mine)
    prod[...] = dot3((c_hi[...], c_lo[...]), split(qtwice[...]))


def y_body(inverse_rows, i0, i1, gathered, own, others, coarse):
    count = gathered.shape[0]
    nmodes, width = coarse.shape
    groups = width // BLOCK

    def part(at, col):
        return gathered[at, col * nmodes : (col + 1) * nmodes]

    blocks = jnp.concatenate(
        [jnp.concatenate([part(at, col) for col in range(groups)], 1) for at in range(count)], 0)
    skip = i0.shape[0] - nmodes
    value = dot6(jnp.concatenate([inverse_rows[...], i0[skip:], i1[skip:]], 0), blocks)
    own[:nmodes] = value[:nmodes]
    others[...] = value[nmodes:]
    tail = gathered[0, groups * nmodes :]
    for at in range(1, count):
        tail = tail + gathered[at, groups * nmodes :]
    own[nmodes:] = jnp.zeros((PAD, width), F32)
    me = lax.axis_index("sub")
    for col in range(groups):
        cols = slice(col * BLOCK, (col + 1) * BLOCK)
        own[nmodes : nmodes + 2, cols] = tail[2 * col : 2 * (col + 1)]
        coarse[:, cols] = part(me, col)


def scalars(sums, rz_old, alpha_old):
    rz, curve = sums[0:1], sums[1:2]
    if rz_old is None:
        return rz / curve, None, rz
    beta = rz / rz_old
    return rz / (curve - beta * rz / alpha_old), beta, rz


def pack(alpha, beta, rz):
    ids = lax.broadcasted_iota(jnp.int32, (PAD, alpha.shape[1]), 0)
    out = jnp.where(ids == 0, alpha, 0.0) + jnp.where(ids == 2, rz, 0.0)
    return out if beta is None else out + jnp.where(ids == 1, beta, 0.0)


def make_image_body(has_old):
    def body(starts, image, prod, k_hi, k_lo, own, others, first, second, *rest):
        *rest, f0, f1, f2, f3 = rest
        nmodes = others.shape[0] // 2
        sums = own[nmodes:] + first[nmodes:] + second[nmodes:]
        if has_old:
            scal_old, along_old, image_new, scal = rest
            alpha, beta, rz = scalars(sums, scal_old[2:3], scal_old[0:1])
        else:
            image_new, along, scal = rest
            alpha, beta, rz = scalars(sums, None, None)
        scal[...] = pack(alpha, beta, rz)
        ys = split(stacked(own, others, first, second))

        @pl.loop(0, image.shape[0] // WIDE)
        def _(at):
            rows = pl.ds(pl.multiple_of(at * WIDE, WIDE), WIDE)
            value = prod[rows, :] + dot3(half((k_hi, k_lo), rows), ys)
            if has_old:
                value = value + beta * along_old[rows, :]
            if not has_old:
                along[rows, :] = value
            image_new[rows, :] = image[rows, :] - alpha * value

        copy_faces(starts, image_new, (f0, f1, f2, f3))

    return body


def make_update_body(has_old, last):
    def body(scal, vee, qtwice, b_hi, b_lo, own, others, first, second,
             resid, qonce, kappa, coarse, eta, image, m_hi, m_lo, *rest):
        if has_old:
            t_old, q_old, k_old, y_old = rest[:4]
            rest = rest[4:]
        if last:
            resid_new, eta_new, q_along, out, vee_new, kappa_new = rest
            t_along = k_along = y_along = None
        else:
            vee_new, resid_new, kappa_new, eta_new, t_along, q_along, k_along, y_along, out = rest
        alpha, beta = scal[0:1], scal[1:2]
        nmodes = kappa.shape[0]
        ys = split(stacked(own, others, first, second))

        def move(old, value, older):
            if has_old:
                value = value + beta * older
            return value, old - alpha * value

        @pl.loop(0, vee.shape[0] // WIDE)
        def _(at):
            rows = pl.ds(pl.multiple_of(at * WIDE, WIDE), WIDE)
            value = qtwice[rows, :] + dot3(half((b_hi, b_lo), rows), ys)
            value, vee_new[rows, :] = move(
                vee[rows, :], value, t_old[rows, :] if has_old else None)
            if not last:
                t_along[rows, :] = value
            q_along[rows, :], resid_new[rows, :] = move(
                resid[rows, :], qonce[rows, :], q_old[rows, :] if has_old else None)

        k_value, kappa_new[...] = move(kappa[...], coarse[...], k_old[...] if has_old else None)
        y_value, eta_new[...] = move(eta[...], own[:nmodes], y_old[...] if has_old else None)
        if not last:
            k_along[...], y_along[...] = k_value, y_value
        moments = moment_rows(vee_new, image, resid_new, kappa_new, eta_new)
        if last:
            for at in range(out.shape[0]):
                out[at] = moments[: out.shape[1]]
        else:
            out[:nmodes] = dot_thin((m_hi[...], m_lo[...]), split(image[...]))
            out[nmodes:] = moments

    return body


def finish_body(starts, sums, scal0, scal1, b_hi, b_lo, e0, e1, e2, r0, r1, r2, along, image,
                g0, g1, g2, g3, answer_out, resid_out, answer, resid, sems):
    nmodes = e0.shape[0]
    order, width = r0.shape
    alpha, beta, _ = scalars(sums[...], scal1[2:3], scal1[0:1])
    a1 = scal1[0:1] + beta * alpha
    a0 = scal0[0:1] + scal1[1:2] * a1
    chunks = [pl.ds(at * TALL, TALL) for at in range(order // TALL)]
    copies = []

    def send(source, target, rows):
        copy = pltpu.make_async_copy(source.at[rows], target.at[rows], sems.at[len(copies)])
        copy.start()
        copies.append(copy)

    ys = split(a0 * e0[...] + a1 * e1[...] + alpha * e2[...])
    for rows in chunks:
        part = dot3((b_hi[rows, :nmodes], b_lo[rows, :nmodes]), ys)
        answer[rows, :] = a0 * r0[rows, :] + a1 * r1[rows, :] + alpha * r2[rows, :] + part
        send(answer, answer_out, rows)
    for rows in chunks:
        resid[rows, :] = r2[rows, :] - alpha * (image[rows, :] + beta * along[rows, :])
    for which, got in enumerate((g0, g1, g2, g3)):
        part = pl.ds(pl.multiple_of(starts[which], BLOCK), BLOCK)
        mask = (0.5 * masks_of(starts, which, width)) * alpha
        resid[part, :] = resid[part, :] - mask * got[...]
    for rows in chunks:
        send(resid, resid_out, rows)
    for copy in copies:
        copy.wait()


def shards(compliance, loads, modes, coarse_inverse, face_block, edge_rows):
    matrix = compliance[0, 0]
    rhs = loads[0, 0]
    basis = modes[0, 0]
    inverse_rows = coarse_inverse[0]
    nmodes, order = basis.shape
    width = rhs.shape[1]
    coarse_all = inverse_rows.shape[1]
    nclus, nsub = lax.axis_size("cluster"), lax.axis_size("sub")
    full = sds(order, width)
    small = sds(nmodes, width)
    block = sds(BLOCK, width)
    tall = 5 * nmodes
    doubled = nclus == 4

    links = [("sub", pair_list(nsub, parity)) for parity in (0, 1)]
    links += [("cluster", pair_list(nclus, parity)) for parity in (0, 1)]

    def exchange(messages):
        got = [None] * 4
        for at in (1, 0, 3, 2):
            got[at] = lax.ppermute(messages[at], links[at][0], links[at][1])
        return got

    def gather(blocks, axis="sub"):
        return lax.all_to_all(blocks, axis, 0, 0, tiled=False)

    def mirror(ymom):
        if doubled:
            second = lax.ppermute(ymom, "cluster", pair_list(nclus, 1, True))
            sums = ymom[nmodes:] + second[nmodes:]
            both = jnp.concatenate([ymom[:nmodes], sums], 0)
            first = lax.ppermute(both, "cluster", pair_list(nclus, 0))
            return first, second
        first = lax.ppermute(ymom, "cluster", pair_list(nclus, 0))
        mine = ymom[nmodes:]
        rest = lax.psum(mine, "cluster") - mine
        second = lax.ppermute(ymom[:nmodes], "cluster", pair_list(nclus, 1))
        return (
            jnp.concatenate([first[:nmodes], rest], 0),
            jnp.concatenate([second, jnp.zeros_like(rest)], 0),
        )

    extra = nmodes * coarse_all // width
    head = BLOCK + nmodes * BLOCK // width
    sizes = [head + (extra if at < 2 else 0) for at in range(4)]
    far = pl.BlockSpec(memory_space=pltpu.HBM)
    *messages, meta, kappa, spread, rhs, basis, flat = pl.pallas_call(
        start_body,
        out_shape=[sds(size, width) for size in sizes]
        + [sds(8, dtype=jnp.int32), small, sds(nsub, nmodes, width), full,
           sds(nmodes, order), sds(extra, width)],
        in_specs=[far] * 5,
        out_specs=[VM] * 4 + [SM] + [VM] * 5,
        scratch_shapes=[
            pltpu.SMEM((nclus, 4, nsub), jnp.int32),
            pltpu.SMEM((nclus, 2, nsub), jnp.int32),
            pltpu.SemaphoreType.DMA((5,)),
        ],
        compiler_params=pltpu.CompilerParams(vmem_limit_bytes=16 << 20),
        name="start",
    )(*(pltpu.with_memory_space_constraint(each, pltpu.HBM) for each in (
        face_block.swapaxes(1, 2), edge_rows.swapaxes(1, 2), rhs, basis,
        inverse_rows.reshape(extra, width))))
    if coarse_all == width:
        inverse_rows = flat
    got = [None] * 2
    for at in (1, 0):
        got[at] = lax.ppermute(messages[at], links[at][0], links[at][1])
    gathered = gather(spread).reshape(nsub * nmodes, width)
    inverses = [inverse_rows, *got]
    if coarse_all != width:
        inverses[1:] = [each[head:].reshape(nmodes, coarse_all) for each in got]
    joined = sds(head + nmodes, width)
    own, *tails = call(
        first_y_body, [small, joined, joined], [inverse_rows, gathered, *messages[2:]])
    second = lax.ppermute(tails[1], "cluster", pair_list(nclus, 1))
    first = lax.ppermute(tails[0], "cluster", pair_list(nclus, 0))
    mapping = sds(order, tall, dtype=BF16)
    thin = sds(nmodes, order, dtype=BF16)
    lates = sds(nmodes, 4 * BLOCK, dtype=BF16)
    args = [meta, pltpu.with_memory_space_constraint(matrix, pltpu.HBM), rhs, basis,
            *inverses[1:], gathered, *got]
    others, *pairs, base, c_hi, c_lo = pl.pallas_call(
        setup_body,
        out_shape=[sds(2 * nmodes, width), mapping, mapping, thin, thin, lates, lates, full]
        + [sds(order, order, dtype=BF16)] * 2,
        in_specs=[SM, far] + [VM] * (len(args) - 2),
        out_specs=[VM] * 10,
        scratch_shapes=[pltpu.VMEM((order, order), F32), pltpu.SemaphoreType.DMA((order // ROWS,))],
        compiler_params=pltpu.CompilerParams(vmem_limit_bytes=16 << 20),
        cost_estimate=pl.CostEstimate(
            flops=100_000_000, bytes_accessed=1 << 22, transcendentals=0),
        name="setup",
    )(*args)
    c_pair = (c_hi, c_lo)
    b_pair, m_pair, l_pair = pairs[0:2], pairs[2:4], pairs[4:6]
    vee, image, *b_pair, f0, f1, f2, f3 = call(
        first_apply_body, [full, full, mapping, mapping] + [block] * 4,
        [meta, base, *c_pair, *b_pair, own, others, first, second], smem_in=(0,))
    own_faces = (f0, f1, f2, f3)
    resid, eta = rhs, own

    resids, etas, scals = [resid], [eta], []
    along = None
    u_along = None
    for step in range(ITERS - 1):
        got = exchange(own_faces)
        if step == 0:
            main = call(sums_body, [sds(nmodes + PAD, width)],
                        [*m_pair, vee, image, resid, kappa, eta])[0]
            k_pair = call(maps_body, [mapping, mapping], [*c_pair, *b_pair],
                          flops=50_000_000)
        else:
            vee, resid, kappa, eta, *along, main = update(False)
            resids.append(resid)
            etas.append(eta)
        spread = call(coarse_late_body, [sds(nsub, (nmodes + 2) * (width // BLOCK), BLOCK)],
                      [main, *l_pair, *got])[0]
        gathered = gather(spread)
        qonce, qtwice, prod = call(
            faces_body, [full, full, full], [meta, image, *c_pair, *got],
            smem_in=(0,), flops=100_000_000)
        own, others, coarse = call(
            y_body, [sds(nmodes + PAD, width), sds(2 * nmodes, width), small],
            [*inverses, gathered])
        first, second = mirror(own)
        old = step > 0
        image_new, *u_next, scal, f0, f1, f2, f3 = call(
            make_image_body(old),
            [full] * (1 if old else 2) + [sds(PAD, width)] + [block] * 4,
            [meta, image, prod, *k_pair, own, others, first, second]
            + ([scals[-1], *u_along] if old else []), smem_in=(0,))
        own_faces, u_along = (f0, f1, f2, f3), u_next
        scals.append(scal)

        def update(last, scal=scal, vee=vee, qtwice=qtwice, own=own, others=others, first=first,
                   second=second, resid=resid, qonce=qonce, kappa=kappa, coarse=coarse, eta=eta,
                   image_new=image_new, along=along, old=old):
            outs = (
                [full, small, full, sds(nclus * nsub, 2, width)]
                if last
                else [full, full, small, small, full, full, small, small,
                      sds(nmodes + PAD, width)]
            )
            return call(
                make_update_body(old, last), outs,
                [scal, vee, qtwice, *b_pair, own, others, first, second, resid, qonce, kappa,
                 coarse, eta, image_new, *m_pair] + (list(along) if old else []),
                scratch=[pltpu.VMEM((order, width), F32), pltpu.VMEM((nmodes, width), F32)]
                if last else ())

        image = image_new

    resid, eta, q_along, main = update(True)
    resids.append(resid)
    etas.append(eta)
    got = exchange(own_faces)
    sums = call(fold_body, [sds(2, width)], [gather(main, ("cluster", "sub"))])[0]
    args = [meta, sums, *scals, *b_pair, *etas, *resids, q_along, image, *got]
    answer, resid = pl.pallas_call(
        finish_body,
        out_shape=[full, full],
        in_specs=[SM] + [VM] * (len(args) - 1),
        out_specs=[far, far],
        scratch_shapes=[
            pltpu.VMEM((order, width), F32),
            pltpu.VMEM((order, width), F32),
            pltpu.SemaphoreType.DMA((2 * order // TALL,)),
        ],
        compiler_params=pltpu.CompilerParams(vmem_limit_bytes=8 << 20),
        cost_estimate=pl.CostEstimate(
            flops=1_000_000, bytes_accessed=1 << 20, transcendentals=0),
        name="finish",
    )(*args)
    return (answer[None, None], resid[None, None])


def solution(mesh):
    return jax.shard_map(
        shards,
        mesh=mesh,
        in_specs=(
            P("cluster", "sub", None, None),
            P("cluster", "sub", None, None),
            P("cluster", "sub", None, None),
            P("cluster", "sub", None),
            P(),
            P(),
        ),
        out_specs=(P("cluster", "sub", None, None), P("cluster", "sub", None, None)),
        check_vma=False,
    )
```
